256 devices in a mesh: nodes: 32 (over y, z_lo, x), orb: 8 (over z_hi, core).
Axes of the slice: x: 4, y: 4, z: 8 (z_hi: 4, z_lo: 2; z = z_hi * 2 + z_lo), core: 2. Of those that a mesh axis runs over, the one named last changes fastest.
Arguments:
- orbitals: float32 [20736, 2048], P('nodes', 'orb'), may hold values from -60 to 60
- cell_matrix: float32 [32, 729, 729], P('nodes'), may hold values from -0.25 to 1.75
- connectivity: int32 [32, 729], P('nodes'), may hold values from 0 to 728, as said below
- face_nodes: int32 [2592], P('nodes'), may hold values from 0 to 647, as said below
Outputs:
- rotated: float32 [20736, 2048], P('nodes', 'orb')
The draws below stay inside these ranges and needn't reach their ends.
Inputs may be any that keep to these rules, and one draw needn't show every extreme that they name: `connectivity`: within a section, entries below 648 are local node numbers and entry 648 + g is ghost slot g; the entries of one cell are distinct, and every local node and every ghost slot of a section appears in some cell of it. Ghost slots appear only in the last cell of a section. `face_nodes`: the 81 entries of a section are distinct local node numbers, listed in the order of the ghost slots of the section below.
All inputs are finite; a program needn't handle non-finite values.
Results may differ from the reference program's by a relative error of at most 0.000088.
Values sent between devices are 32-bit elements; how exact they have to be, the bound alone decides.
A program may use at most 64 MiB of HBM per device.

```python
import math
import jax
import jax.numpy as jnp
from jax import lax

SIDE = 9
ORBS = 2048
DEGREE = 8
CELLS_DEV = 1
CELL_NODES = 729
FACE = 81
NODES_DEV = 648
NODES = 20736
CELLS = 32
N_NODES = 32


def section_perms(key):
    sections = CELLS // CELLS_DEV
    keys = jax.random.split(jax.random.fold_in(key, 11), sections)
    return jax.vmap(lambda sub: jax.random.permutation(sub, NODES_DEV))(keys).astype(jnp.int32)


def draw_connectivity(key, part):
    perms = section_perms(key)
    layers = (SIDE - 1) * CELLS_DEV
    cell = jnp.arange(CELLS, dtype=jnp.int32)
    section = cell // CELLS_DEV
    within = cell % CELLS_DEV
    node = jnp.arange(CELL_NODES, dtype=jnp.int32)
    first = node // FACE
    second = node // SIDE % SIDE
    third = node % SIDE
    plane = first * SIDE + second
    layer = within[:, None] * (SIDE - 1) + third[None, :]
    structured = layer * FACE + plane[None, :]
    local = perms[section[:, None], jnp.minimum(structured, NODES_DEV - 1)]
    return jnp.where(layer < layers, local, NODES_DEV + plane[None, :]).astype(jnp.int32)


def draw_face_nodes(key, part):
    perms = section_perms(key)
    return perms[:, :FACE].reshape(-1).astype(jnp.int32)


def draw_cell_matrix(key, part):
    first, second = jax.random.split(jax.random.fold_in(key, 5), 2)
    spread = 0.25 / math.sqrt(CELL_NODES)
    noise = jnp.clip(jax.random.normal(first, (CELLS, CELL_NODES, CELL_NODES), jnp.float32), -3.0, 3.0)
    symmetric = (noise + jnp.swapaxes(noise, 1, 2)) * (spread / math.sqrt(2.0))
    diagonal = jnp.exp(jax.random.uniform(second, (CELLS, CELL_NODES), jnp.float32, math.log(0.3), math.log(1.5)))
    return symmetric + diagonal[:, :, None] * jnp.eye(CELL_NODES, dtype=jnp.float32)[None]


def draw_orbitals(key, part):
    first, second, third = jax.random.split(jax.random.fold_in(key, 3), 3)
    base = jnp.clip(jax.random.normal(first, (NODES, ORBS), jnp.float32), -4.0, 4.0)
    position = jnp.arange(NODES, dtype=jnp.float32) / max(NODES - 1, 1)
    rising = jnp.sqrt(1.0 + 2.0 * position) * jnp.exp(jax.random.uniform(second, (NODES,), jnp.float32, -0.4, 0.4))
    columns = jnp.exp(jax.random.uniform(third, (ORBS,), jnp.float32, -0.4, 0.4))
    return base * rising[:, None] * columns[None, :]


def setup_inputs(seed: int = 0) -> dict:
    splits = jax.random.split(jax.random.key(seed), 5)
    orbitals = draw_orbitals(jax.random.fold_in(splits[4], 71), 0)
    cell_matrix = draw_cell_matrix(jax.random.fold_in(splits[4], 71), 0)
    connectivity = draw_connectivity(jax.random.fold_in(splits[4], 71), 0)
    face_nodes = draw_face_nodes(jax.random.fold_in(splits[4], 71), 0)
    return {"orbitals": orbitals, "cell_matrix": cell_matrix, "connectivity": connectivity, "face_nodes": face_nodes}


lowest = -1.0
cutoff = 1.5
ceiling = 4.5
eps_norm = 1e-06

def chebyshev(start, apply_fn):
    half_width = (ceiling - cutoff) / 2.0
    centre = (ceiling + cutoff) / 2.0
    sigma_one = half_width / (lowest - centre)
    prev = start
    cur = (apply_fn(prev) - centre * prev) * (sigma_one / half_width)
    sigma_now = sigma_one
    for degree_step in range(DEGREE - 1):
        sigma_next = 1.0 / (2.0 / sigma_one - sigma_now)
        fresh = (apply_fn(cur) - centre * cur) * (2.0 * sigma_next / half_width) - sigma_now * sigma_next * prev
        prev = cur
        cur = fresh
        sigma_now = sigma_next
    return cur

def reference(orbitals, cell_matrix, connectivity, face_nodes):
    section = (jnp.arange(CELLS, dtype=jnp.int32) // CELLS_DEV)[:, None]
    face_all = face_nodes.reshape(N_NODES, FACE)
    above = jnp.minimum(section + 1, N_NODES - 1).astype(jnp.int32)
    slot = jnp.clip(connectivity - NODES_DEV, 0, FACE - 1).astype(jnp.int32)
    ghost_target = (section + 1) * NODES_DEV + face_all[above, slot]
    has_above = section + 1 < N_NODES
    global_index = jnp.where(connectivity < NODES_DEV, section * NODES_DEV + connectivity, jnp.where(has_above, ghost_target, NODES)).astype(jnp.int32)
    flat_index = global_index.reshape(-1)

    def apply_ham(field):
        extended = jnp.concatenate([field, jnp.zeros((1, ORBS), jnp.float32)], axis=0)
        local = extended[global_index]
        product = jnp.einsum('cij,cjo->cio', cell_matrix, local, precision=lax.Precision.HIGHEST)
        summed = jnp.zeros((NODES + 1, ORBS), jnp.float32).at[flat_index].add(product.reshape(-1, ORBS))
        return summed[:NODES]
    filtered = chebyshev(orbitals, apply_ham)
    intersection = jnp.dot(filtered.T, filtered, precision=lax.Precision.HIGHEST)
    scale = lax.rsqrt(jnp.diagonal(intersection) / NODES + eps_norm)
    unit = filtered * scale[None, :]
    coupling = intersection * scale[:, None] * scale[None, :] / NODES
    return 1.5 * unit - 0.5 * jnp.dot(unit, coupling, precision=lax.Precision.HIGHEST)
```

```python
import functools

import jax
import jax.numpy as jnp
from jax import lax
from jax.experimental import pallas as pl
from jax.experimental.pallas import tpu as pltpu
from jax.sharding import PartitionSpec as P

DEGREE = 8
lowest = -1.0
cutoff = 1.5
ceiling = 4.5
eps_norm = 1e-06

F32 = jnp.float32
BF16 = jnp.bfloat16
MESH = pl.DeviceIdType.MESH

OWN = 648
CELL = 729
FACE = 81
TOTAL_ROWS = 20736
W = 256
HALF = 128
KP = 768
LOW = 567
REG_L = 560
REG_G = 648
REG = 88
REG_END = 736
INT = 560
CUT = 512
ROWS = 656
PART = 320


def coefficients():
    half_width = (ceiling - cutoff) / 2.0
    centre = (ceiling + cutoff) / 2.0
    sigma_one = half_width / (lowest - centre)
    table = [(sigma_one / half_width, 0.0)]
    now = sigma_one
    for _ in range(DEGREE - 1):
        nxt = 1.0 / (2.0 / sigma_one - now)
        table.append((2.0 * nxt / half_width, now * nxt))
        now = nxt
    return centre, table


CENTRE, TABLE = coefficients()


def chosen(t, which):
    if isinstance(t, int):
        return TABLE[t][which]
    value = jnp.float32(TABLE[0][which])
    for step in range(1, DEGREE):
        value = jnp.where(t == step, jnp.float32(TABLE[step][which]), value)
    return value


def split2(value):
    high = value.astype(BF16)
    low = (value - high.astype(F32)).astype(BF16)
    return high, low


def dot(left, right):
    return jnp.dot(left, right, preferred_element_type=F32)


def dot_nt(left, right):
    return lax.dot_general(left, right, (((1,), (1,)), ((), ())), preferred_element_type=F32)


def iota(shape, dim):
    return lax.broadcasted_iota(jnp.int32, shape, dim)


def one_hot(position, shape, dim):
    return jnp.where(iota(shape, dim).astype(F32) == position, 1.0, 0.0).astype(BF16)


def kernel(
    x_ref, a_ref, conn_ref, faces_ref, out_ref,
    irow, q, ah, al, bh, bl, mh, ml, qt, vcat, vbuf, xs, pre, pf,
    send_l, send_g, from_above, from_below,
    fall, ta_h, ta_l, tb_h, tb_l, stage_h, stage_l, acc, rot_h, rot_l,
    tiles, arrived, mine, ex0, ex1, ex2, final, gathered, norms, nown, scales,
    halo_send, halo_recv, z_send, z_recv, d_send, d_recv,
    rs_send, rs_recv, ex_send, ex_recv, ag_send, ag_recv, n_send, n_recv, s_send, s_recv,
):
    node = lax.axis_index("nodes")
    orb = lax.axis_index("orb")
    a = orb // 2
    c = orb % 2
    zl = (node // 4) % 2
    xy = (node // 8) * 4 + node % 4
    flip = node + 4 - 8 * zl
    up = (node + 1) % 32
    down = (node + 31) % 32
    has_above = jnp.where(node < 31, jnp.float32(1.0), jnp.float32(0.0))
    has_below = jnp.where(node > 0, jnp.float32(1.0), jnp.float32(0.0))

    def orb_at(da, dc):
        other = c if dc == 0 else 1 - c
        return ((a + da) % 4) * 2 + other

    def node_of(position, z):
        return (position // 4) * 8 + z * 4 + position % 4

    barrier = pltpu.get_barrier_semaphore()

    def greet(k, _):
        pl.semaphore_signal(barrier, inc=1, device_id=((node + k) % 32, orb), device_id_type=MESH)
        return 0

    lax.fori_loop(1, 32, greet, 0)
    for k in range(1, 8):
        pl.semaphore_signal(barrier, inc=1, device_id=(node, orb_at(k // 2, k % 2)), device_id_type=MESH)
    for k in range(2, 8):
        pl.semaphore_signal(barrier, inc=1, device_id=(flip, orb_at(k // 2, k % 2)), device_id_type=MESH)

    irow[...] = jnp.full(irow.shape, 100000, jnp.int32)
    irow[0:1, 0:FACE] = faces_ref[...]
    face_row = irow[0:1, 0:128].astype(F32)
    irow[8:9, 0:CELL] = conn_ref[...]
    entry = irow[8:9, :].astype(F32)
    square = (128, 128)
    face_col = jnp.sum(
        jnp.where(iota(square, 0) == iota(square, 1), jnp.broadcast_to(face_row, square), 0.0), axis=1, keepdims=True
    )

    def position_row(number):
        shape = (128, KP)
        same = number == face_col
        hit = jnp.sum(jnp.where(same, iota(shape, 0).astype(F32) + 1.0, 0.0), axis=0, keepdims=True)
        below = jnp.sum(jnp.where(face_col < number, 1.0, 0.0), axis=0, keepdims=True)
        return jnp.where(hit > 0.0, LOW - 1.0 + hit, number - below)

    local = iota((1, KP), 1).astype(F32)
    local_pos = jnp.where(local < OWN, position_row(local), -1.0)
    cell_pos = jnp.where(entry < OWN, position_row(entry), jnp.where(entry < CELL, entry + 7.0, -1.0))

    q[...] = one_hot(local_pos, (KP, KP), 0)
    xs[...] = jnp.zeros(xs.shape, F32)
    xs[0:OWN, :] = x_ref[...]
    start = xs[...]
    x1 = start.astype(BF16)
    rest = start - x1.astype(F32)
    x2 = rest.astype(BF16)
    x3 = (rest - x2.astype(F32)).astype(BF16)
    vbuf[0, ...] = (dot(q[...], x1) + dot(q[...], x2)) + dot(q[...], x3)
    vbuf[1, ...] = jnp.zeros((KP, W), F32)

    pl.semaphore_wait(barrier, 31 + 7 + 6)

    def columns(chunk):
        return slice(chunk * HALF, (chunk + 1) * HALF)

    def halo(t, chunk, way):
        slot = (t + 2) % 2
        if way == 0:
            src, dst, target = send_l, from_above, down
        else:
            src, dst, target = send_g, from_below, up
        return pltpu.make_async_remote_copy(
            src_ref=src.at[slot, chunk],
            dst_ref=dst.at[slot, chunk],
            send_sem=halo_send.at[slot, chunk, way],
            recv_sem=halo_recv.at[slot, chunk, way],
            device_id=(target, orb),
            device_id_type=MESH,
        )

    for chunk in range(2):
        send_l[1, chunk] = vbuf[0, REG_L:REG_G, columns(chunk)]
        halo(-1, chunk, 0).start()

    q[...] = one_hot(cell_pos, (KP, KP), 0)
    xs_rows = a_ref[...]
    high, low = split2(xs_rows)
    ah[...] = jnp.zeros(ah.shape, BF16)
    al[...] = jnp.zeros(al.shape, BF16)
    ah[0:CELL, 0:CELL] = high
    al[0:CELL, 0:CELL] = low
    bh[...] = dot(q[...], ah[...]).astype(BF16)
    bl[...] = dot(q[...], al[...]).astype(BF16)
    mh[...] = dot_nt(bh[...], q[...]).astype(BF16)
    ml[...] = dot_nt(bl[...], q[...]).astype(BF16)

    reg_row = iota((REG, HALF), 0)
    mask = jnp.where(reg_row >= 7, 1.0, 0.0).astype(F32) * has_above

    def put(chunk, low_row, high_row, value):
        high, low = split2(value)
        vcat[chunk, low_row:high_row, 0:HALF] = high
        vcat[chunk, low_row:high_row, HALF:W] = low

    def product(chunk, rows, depth):
        both = dot(mh[rows, depth], vcat[chunk, depth, :])
        third = dot(ml[rows, depth], vcat[chunk, depth, 0:HALF])
        return (both[:, 0:HALF] + both[:, HALF:W]) + third

    def prepare(chunk):
        pre[chunk] = product(chunk, slice(INT, REG_END), slice(0, CUT))

    for chunk in range(2):
        put(chunk, 0, KP, vbuf[0, :, columns(chunk)])
        prepare(chunk)

    def faces_out(t, chunk):
        value = pre[chunk] + product(chunk, slice(INT, REG_END), slice(CUT, KP))
        pf[chunk] = value
        slot = (t + 2) % 2
        send_l[slot, chunk] = value[0:REG]
        send_g[slot, chunk] = value[REG : 2 * REG]
        halo(t, chunk, 0).start()
        halo(t, chunk, 1).start()

    def interior(t, chunk):
        now, old = t % 2, (t + 1) % 2
        total = product(chunk, slice(0, INT), slice(0, KP))
        cols = columns(chunk)
        fresh = (total - CENTRE * vbuf[now, 0:INT, cols]) * chosen(t, 0) - chosen(t, 1) * vbuf[old, 0:INT, cols]
        vbuf[old, 0:INT, cols] = fresh
        put(chunk, 0, INT, fresh)

    def faces_in(t, chunk):
        now, old = t % 2, (t + 1) % 2
        slot = t % 2
        halo(t, chunk, 0).wait_recv()
        halo(t, chunk, 1).wait_recv()
        cols = columns(chunk)
        lower = pf[chunk, 0:REG] + from_below[slot, chunk] * has_below
        upper = (pf[chunk, REG : 2 * REG] + from_above[slot, chunk]) * mask
        for rows, total in ((slice(REG_L, REG_G), lower), (slice(REG_G, REG_END), upper)):
            fresh = (total - CENTRE * vbuf[now, rows, cols]) * chosen(t, 0) - chosen(t, 1) * vbuf[old, rows, cols]
            vbuf[old, rows, cols] = fresh
            put(chunk, rows.start, rows.stop, fresh)

    def close(t):
        for chunk in range(2):
            halo(t, chunk, 0).wait_send()
            halo(t, chunk, 1).wait_send()

    for chunk in range(2):
        halo(-1, chunk, 0).wait_recv()
        ghost = from_above[1, chunk] * mask
        vbuf[0, REG_G:REG_END, columns(chunk)] = ghost
        put(chunk, REG_G, REG_END, ghost)
        faces_out(0, chunk)
    for chunk in range(2):
        interior(0, chunk)
        prepare(chunk)
    for chunk in range(2):
        halo(-1, chunk, 0).wait_send()
    close(0)

    def step(t, _):
        for chunk in range(2):
            faces_in(t - 1, chunk)
            faces_out(t, chunk)
        for chunk in range(2):
            interior(t, chunk)
            prepare(chunk)
        close(t)
        return 0

    lax.fori_loop(1, DEGREE, step, 0)
    for chunk in range(2):
        faces_in(DEGREE - 1, chunk)

    fall[0, 0:OWN, :] = vbuf[DEGREE % 2, 0:OWN, :]
    own = fall[0, 0:OWN, :]
    nown[0] = jnp.sum(own * own, axis=0, keepdims=True)
    norms[node] = nown[0]

    def norm_copy(k):
        return pltpu.make_async_remote_copy(
            src_ref=nown.at[0],
            dst_ref=norms.at[node],
            send_sem=n_send,
            recv_sem=n_recv,
            device_id=((node + k) % 32, orb),
            device_id_type=MESH,
        )

    def norm_start(k, _):
        norm_copy(k).start()
        return 0

    lax.fori_loop(1, 32, norm_start, 0)

    first, second = slice(0, PART), slice(PART, OWN)

    def z_copy(index):
        src, dst, rows, da = (
            (0, 6, first, 1),
            (0, 2, second, -1),
            (6, 4, first, 1),
            (2, 4, second, -1),
            (0, 6, second, 1),
            (0, 2, first, -1),
        )[index]
        return pltpu.make_async_remote_copy(
            src_ref=fall.at[src, rows],
            dst_ref=fall.at[dst, rows],
            send_sem=z_send.at[index],
            recv_sem=z_recv.at[index],
            device_id=(node, orb_at(da, 0)),
            device_id_type=MESH,
        )

    def d_copy(index):
        slot, rows = (
            (0, slice(0, OWN)),
            (6, first),
            (2, second),
            (4, first),
            (4, second),
            (6, second),
            (2, first),
        )[index]
        return pltpu.make_async_remote_copy(
            src_ref=fall.at[slot, rows],
            dst_ref=fall.at[slot + 1, rows],
            send_sem=d_send.at[index],
            recv_sem=d_recv.at[index],
            device_id=(node, orb_at(0, 1)),
            device_id_type=MESH,
        )

    z_copy(0).start()
    z_copy(1).start()
    d_copy(0).start()
    for k in range(8):
        fall[k, OWN:ROWS, :] = jnp.zeros((ROWS - OWN, W), F32)
    stage_h[...] = jnp.zeros(stage_h.shape, BF16)
    stage_l[...] = jnp.zeros(stage_l.shape, BF16)

    padded = (384, W)
    top = jnp.where(iota(padded, 0) < PART, fall[0, 0:384, :], 0.0)
    ta_h[...], ta_l[...] = split2(top.T)
    xs[...] = jnp.zeros(xs.shape, F32)
    xs[0 : OWN - PART, :] = fall[0, PART:OWN, :]
    tb_h[...], tb_l[...] = split2(xs[0:384, :].T)

    def half_gram(which, slot):
        rows = first if which == 0 else second
        high, low = split2(fall[slot, rows, :])
        count = rows.stop - rows.start
        stage_h[which, 0:count, :] = high
        stage_l[which, 0:count, :] = low
        left_h, left_l = (ta_h, ta_l) if which == 0 else (tb_h, tb_l)
        return (dot(left_h[...], stage_h[which]) + dot(left_h[...], stage_l[which])) + dot(left_l[...], stage_h[which])

    def keep(tile, value):
        tiles[tile] = value.reshape(16, 16, W)

    def rs_copy(group, k):
        lo, hi = ((0, 2), (2, 6), (6, 7))[group]
        other = xy ^ k
        return pltpu.make_async_remote_copy(
            src_ref=tiles.at[lo:hi, other],
            dst_ref=arrived.at[lo:hi, xy],
            send_sem=rs_send.at[group],
            recv_sem=rs_recv.at[group],
            device_id=(node_of(other, zl), orb),
            device_id_type=MESH,
        )

    def rs_start(group):
        def one(k, _):
            rs_copy(group, k).start()
            return 0

        lax.fori_loop(1, 16, one, 0)

    def rs_sum(group):
        lo, hi = ((0, 2), (2, 6), (6, 7))[group]
        whole = arrived.at[lo:hi, 0:15]
        pltpu.make_async_copy(whole, whole, rs_recv.at[group]).wait()
        for tile in range(lo, hi):
            arrived[tile, xy] = tiles[tile, xy]
            mine[tile] = jnp.sum(arrived[tile], axis=0)

    keep(0, half_gram(0, 0) + half_gram(1, 0))
    d_copy(0).wait_recv()
    keep(1, half_gram(0, 1) + half_gram(1, 1))
    rs_start(0)

    whole_norms = norms.at[0:31]
    pltpu.make_async_copy(whole_norms, whole_norms, n_recv).wait()
    scales[0] = lax.rsqrt(jnp.sum(norms[...], axis=0) / TOTAL_ROWS + eps_norm)

    def scale_copy(k):
        da, dc = k // 2, k % 2
        return pltpu.make_async_remote_copy(
            src_ref=scales.at[0],
            dst_ref=scales.at[((4 - da) % 4) * 2 + dc],
            send_sem=s_send.at[k],
            recv_sem=s_recv.at[k],
            device_id=(node, orb_at(da, dc)),
            device_id_type=MESH,
        )

    for k in range(1, 8):
        scale_copy(k).start()

    z_copy(0).wait_recv()
    z_copy(2).start()
    d_copy(1).start()
    z_copy(1).wait_recv()
    z_copy(3).start()
    d_copy(2).start()
    keep(2, half_gram(0, 6))
    keep(4, half_gram(1, 2).T)
    d_copy(1).wait_recv()
    keep(3, half_gram(0, 7))
    d_copy(2).wait_recv()
    keep(5, half_gram(1, 3).T)
    rs_start(1)
    rs_sum(0)

    z_copy(2).wait_recv()
    d_copy(3).start()
    z_copy(3).wait_recv()
    d_copy(4).start()
    d_copy(3).wait_recv()
    d_copy(4).wait_recv()
    late = jnp.where(a >= 2, 1, 0)
    keep(6, half_gram(0, 4 + late) + half_gram(1, 4 + late))
    rs_start(2)
    rs_sum(1)
    rs_sum(2)

    cross = jnp.where(a >= 2, 1 - c, c)
    partner = ((a + 2) % 4) * 2 + cross
    pairs = (
        (2, 4, orb_at(-1, 0)),
        (3, 5, orb_at(-1, 1)),
        (4, 2, orb_at(1, 0)),
        (5, 3, orb_at(1, 1)),
        (6, 7, partner),
    )

    def ex_copies():
        copies = [
            pltpu.make_async_remote_copy(
                src_ref=mine.at[0:7],
                dst_ref=ex0,
                send_sem=ex_send.at[0],
                recv_sem=ex_recv.at[0],
                device_id=(flip, orb),
                device_id_type=MESH,
            )
        ]
        for index, (src, dst, who) in enumerate(pairs):
            for near in range(2):
                copies.append(
                    pltpu.make_async_remote_copy(
                        src_ref=mine.at[src],
                        dst_ref=(ex1, ex2)[near].at[dst],
                        send_sem=ex_send.at[1 + 2 * index + near],
                        recv_sem=ex_recv.at[1 + 2 * (dst if dst < 7 else 6) - 4 + near],
                        device_id=(node if near == 0 else flip, who),
                        device_id_type=MESH,
                    )
                )
        return copies

    exchange = ex_copies()
    for copy in exchange:
        copy.start()
    z_copy(4).start()
    z_copy(5).start()
    for copy in exchange:
        copy.wait_recv()
    for tile in range(8):
        if tile < 2 or tile == 6:
            final[tile] = mine[tile] + ex0[tile]
        elif tile == 7:
            final[tile] = ex1[tile] + ex2[tile]
        else:
            final[tile] = (mine[tile] + ex0[tile]) + (ex1[tile] + ex2[tile])
        gathered[tile, xy] = final[tile]

    def ag_copy(k):
        return pltpu.make_async_remote_copy(
            src_ref=final,
            dst_ref=gathered.at[0:8, xy],
            send_sem=ag_send,
            recv_sem=ag_recv,
            device_id=(node_of(xy ^ k, zl), orb),
            device_id_type=MESH,
        )

    def ag_start(k, _):
        ag_copy(k).start()
        return 0

    lax.fori_loop(1, 16, ag_start, 0)

    natural = iota((ROWS, 1), 0).astype(F32)
    face_lane = jnp.broadcast_to(face_row, (ROWS, 128))
    lane = iota((ROWS, 128), 1).astype(F32)
    hit = jnp.sum(jnp.where(face_lane == natural, lane + 1.0, 0.0), axis=1, keepdims=True)
    below = jnp.sum(jnp.where(face_lane < natural, 1.0, 0.0), axis=1, keepdims=True)
    back = jnp.where(hit > 0.0, LOW - 1.0 + hit, natural - below)
    qt[...] = one_hot(back, (ROWS, KP), 1)
    rot_h[ROWS:KP, :] = jnp.zeros((KP - ROWS, W), BF16)
    rot_l[ROWS:KP, :] = jnp.zeros((KP - ROWS, W), BF16)

    for k in range(1, 8):
        scale_copy(k).wait_recv()
    z_copy(4).wait_recv()
    d_copy(5).start()
    z_copy(5).wait_recv()
    d_copy(6).start()
    whole_tiles = gathered.at[0:8, 0:15]
    pltpu.make_async_copy(whole_tiles, whole_tiles, ag_recv).wait()

    def rotated(slot, tile, transposed):
        scale = scales[slot]
        left_h, left_l = split2(fall[slot] * (scale * scale))
        right_h, right_l = split2(gathered[tile].reshape(W, W))
        times = dot_nt if transposed else dot
        return (times(left_h, right_h) + times(left_h, right_l)) + times(left_l, right_h)

    acc[...] = rotated(0, 0, False)
    acc[...] += rotated(1, 1, True)
    acc[...] += rotated(4 + late, 6, True)
    acc[...] += rotated(5 - late, 7, False)
    acc[...] += rotated(2, 4, False)
    acc[...] += rotated(6, 2, True)
    d_copy(5).wait_recv()
    acc[...] += rotated(7, 3, True)
    d_copy(6).wait_recv()
    acc[...] += rotated(3, 5, False)
    result = (1.5 * fall[0] - (0.5 / TOTAL_ROWS) * acc[...]) * scales[0]
    high, low = split2(result)
    rot_h[0:ROWS, :] = high
    rot_l[0:ROWS, :] = low
    out = dot(qt[...], rot_h[...]) + dot(qt[...], rot_l[...])
    out_ref[...] = out[0:OWN, :]

    for index in range(6):
        z_copy(index).wait_send()
    for index in range(7):
        d_copy(index).wait_send()
    for k in range(1, 8):
        scale_copy(k).wait_send()
    pltpu.make_async_copy(whole_norms, whole_norms, n_send).wait()
    for group, (lo, hi) in enumerate(((0, 2), (2, 6), (6, 7))):
        whole = arrived.at[lo:hi, 0:15]
        pltpu.make_async_copy(whole, whole, rs_send.at[group]).wait()
    for copy in exchange:
        copy.wait_send()
    pltpu.make_async_copy(whole_tiles, whole_tiles, ag_send).wait()


def body(orbitals, cell_matrix, connectivity, face_nodes):
    vmem = pl.BlockSpec(memory_space=pltpu.VMEM)
    dma = pltpu.SemaphoreType.DMA
    return pl.pallas_call(
        kernel,
        out_shape=jax.ShapeDtypeStruct((OWN, W), F32),
        in_specs=[vmem] * 4,
        out_specs=vmem,
        scratch_shapes=[
            pltpu.VMEM((16, KP), jnp.int32),
            pltpu.VMEM((KP, KP), BF16),
            pltpu.VMEM((KP, KP), BF16),
            pltpu.VMEM((KP, KP), BF16),
            pltpu.VMEM((KP, KP), BF16),
            pltpu.VMEM((KP, KP), BF16),
            pltpu.VMEM((KP, KP), BF16),
            pltpu.VMEM((KP, KP), BF16),
            pltpu.VMEM((ROWS, KP), BF16),
            pltpu.VMEM((2, KP, W), BF16),
            pltpu.VMEM((2, KP, W), F32),
            pltpu.VMEM((KP, W), F32),
            pltpu.VMEM((2, 2 * REG, HALF), F32),
            pltpu.VMEM((2, 2 * REG, HALF), F32),
            pltpu.VMEM((2, 2, REG, HALF), F32),
            pltpu.VMEM((2, 2, REG, HALF), F32),
            pltpu.VMEM((2, 2, REG, HALF), F32),
            pltpu.VMEM((2, 2, REG, HALF), F32),
            pltpu.VMEM((8, ROWS, W), F32),
            pltpu.VMEM((W, 384), BF16),
            pltpu.VMEM((W, 384), BF16),
            pltpu.VMEM((W, 384), BF16),
            pltpu.VMEM((W, 384), BF16),
            pltpu.VMEM((2, 384, W), BF16),
            pltpu.VMEM((2, 384, W), BF16),
            pltpu.VMEM((ROWS, W), F32),
            pltpu.VMEM((KP, W), BF16),
            pltpu.VMEM((KP, W), BF16),
            pltpu.VMEM((7, 16, 16, W), F32),
            pltpu.VMEM((7, 16, 16, W), F32),
            pltpu.VMEM((7, 16, W), F32),
            pltpu.VMEM((7, 16, W), F32),
            pltpu.VMEM((8, 16, W), F32),
            pltpu.VMEM((8, 16, W), F32),
            pltpu.VMEM((8, 16, W), F32),
            pltpu.VMEM((8, 16, 16, W), F32),
            pltpu.VMEM((32, 1, W), F32),
            pltpu.VMEM((1, 1, W), F32),
            pltpu.VMEM((8, 1, W), F32),
            dma((2, 2, 2)),
            dma((2, 2, 2)),
            dma((6,)),
            dma((6,)),
            dma((7,)),
            dma((7,)),
            dma((3,)),
            dma((3,)),
            dma((11,)),
            dma((11,)),
            dma,
            dma,
            dma,
            dma,
            dma((8,)),
            dma((8,)),
        ],
        compiler_params=pltpu.CompilerParams(
            collective_id=0, has_side_effects=True, vmem_limit_bytes=60 * 1024 * 1024
        ),
    )(orbitals, cell_matrix[0], connectivity, face_nodes.reshape(1, FACE))


def solution(mesh):
    return jax.shard_map(
        body,
        mesh=mesh,
        in_specs=(P("nodes", "orb"), P("nodes", None, None), P("nodes", None), P("nodes")),
        out_specs=P("nodes", "orb"),
        check_vma=False,
    )
```

```python
import functools

import jax
import jax.numpy as jnp
from jax import lax
from jax.experimental import pallas as pl
from jax.experimental.pallas import tpu as pltpu
from jax.sharding import PartitionSpec as P

DEGREE = 8
lowest = -1.0
cutoff = 1.5
ceiling = 4.5
eps_norm = 1e-06

F32 = jnp.float32
BF16 = jnp.bfloat16
MESH = pl.DeviceIdType.MESH

OWN = 648
CELL = 729
FACE = 81
TOTAL_ROWS = 20736
W = 256
HALF = 128
KP = 768
LOW = 567
REG_L = 560
REG_G = 648
REG = 88
REG_END = 736
INT = 560
CUT = 512
ROWS = 656
PART = 320


def coefficients():
    half_width = (ceiling - cutoff) / 2.0
    centre = (ceiling + cutoff) / 2.0
    sigma_one = half_width / (lowest - centre)
    table = [(sigma_one / half_width, 0.0)]
    now = sigma_one
    for _ in range(DEGREE - 1):
        nxt = 1.0 / (2.0 / sigma_one - now)
        table.append((2.0 * nxt / half_width, now * nxt))
        now = nxt
    return centre, table


CENTRE, TABLE = coefficients()


def chosen(t, which):
    if isinstance(t, int):
        return TABLE[t][which]
    value = jnp.float32(TABLE[0][which])
    for step in range(1, DEGREE):
        value = jnp.where(t == step, jnp.float32(TABLE[step][which]), value)
    return value


def split2(value):
    high = value.astype(BF16)
    low = (value - high.astype(F32)).astype(BF16)
    return high, low


def dot(left, right):
    return jnp.dot(left, right, preferred_element_type=F32)


def dot_nt(left, right):
    return lax.dot_general(left, right, (((1,), (1,)), ((), ())), preferred_element_type=F32)


def iota(shape, dim):
    return lax.broadcasted_iota(jnp.int32, shape, dim)


def one_hot(position, shape, dim):
    return jnp.where(iota(shape, dim).astype(F32) == position, 1.0, 0.0).astype(BF16)


def kernel(
    x_ref, a_ref, conn_ref, faces_ref, out_ref,
    irow, q, ah, al, bh, bl, mh, ml, qt, vcat, vbuf, xs, pre, pf,
    send_l, send_g, from_above, from_below,
    fall, ta_h, ta_l, tb_h, tb_l, stage_h, stage_l, acc, rot_h, rot_l,
    flat, flat_in, cube, cube_in, mine, ex0, ex1, ex2, final, gathered, gathered_flat, norms, nown, scales,
    halo_send, halo_recv, z_send, z_recv, d_send, d_recv,
    rs_send, rs_recv, c_send, c_recv, g_send, g_recv, ex_send, ex_recv, ag_send, ag_recv, n_send, n_recv, s_send, s_recv,
):
    node = lax.axis_index("nodes")
    orb = lax.axis_index("orb")
    a = orb // 2
    c = orb % 2
    zl = (node // 4) % 2
    x, y = node % 4, node // 8
    bits = ((x // 2 + x % 2) % 2, x // 2, (y // 2 + y % 2) % 2, y // 2)
    flip = node + 4 - 8 * zl
    up = (node + 1) % 32
    down = (node + 31) % 32
    has_above = jnp.where(node < 31, jnp.float32(1.0), jnp.float32(0.0))
    has_below = jnp.where(node > 0, jnp.float32(1.0), jnp.float32(0.0))

    def orb_at(da, dc):
        other = c if dc == 0 else 1 - c
        return ((a + da) % 4) * 2 + other

    def number(corner):
        return corner[3] * 8 + corner[2] * 4 + corner[1] * 2 + corner[0]

    def node_of(corner):
        there_x = corner[1] * 2 + (corner[0] + corner[1]) % 2
        there_y = corner[3] * 2 + (corner[2] + corner[3]) % 2
        return there_y * 8 + zl * 4 + there_x

    sid = number(bits)

    barrier = pltpu.get_barrier_semaphore()

    def greet(k, _):
        pl.semaphore_signal(barrier, inc=1, device_id=((node + k) % 32, orb), device_id_type=MESH)
        return 0

    lax.fori_loop(1, 32, greet, 0)
    for k in range(1, 8):
        pl.semaphore_signal(barrier, inc=1, device_id=(node, orb_at(k // 2, k % 2)), device_id_type=MESH)
    for k in range(2, 8):
        pl.semaphore_signal(barrier, inc=1, device_id=(flip, orb_at(k // 2, k % 2)), device_id_type=MESH)

    irow[...] = jnp.full(irow.shape, 100000, jnp.int32)
    irow[0:1, 0:FACE] = faces_ref[...]
    face_row = irow[0:1, 0:128].astype(F32)
    irow[8:9, 0:CELL] = conn_ref[...]
    entry = irow[8:9, :].astype(F32)
    square = (128, 128)
    face_col = jnp.sum(
        jnp.where(iota(square, 0) == iota(square, 1), jnp.broadcast_to(face_row, square), 0.0), axis=1, keepdims=True
    )

    def position_row(number):
        shape = (128, KP)
        same = number == face_col
        hit = jnp.sum(jnp.where(same, iota(shape, 0).astype(F32) + 1.0, 0.0), axis=0, keepdims=True)
        below = jnp.sum(jnp.where(face_col < number, 1.0, 0.0), axis=0, keepdims=True)
        return jnp.where(hit > 0.0, LOW - 1.0 + hit, number - below)

    local = iota((1, KP), 1).astype(F32)
    local_pos = jnp.where(local < OWN, position_row(local), -1.0)
    cell_pos = jnp.where(entry < OWN, position_row(entry), jnp.where(entry < CELL, entry + 7.0, -1.0))

    q[...] = one_hot(local_pos, (KP, KP), 0)
    xs[...] = jnp.zeros(xs.shape, F32)
    xs[0:OWN, :] = x_ref[...]
    start = xs[...]
    x1 = start.astype(BF16)
    rest = start - x1.astype(F32)
    x2 = rest.astype(BF16)
    x3 = (rest - x2.astype(F32)).astype(BF16)
    vbuf[0, ...] = (dot(q[...], x1) + dot(q[...], x2)) + dot(q[...], x3)
    vbuf[1, ...] = jnp.zeros((KP, W), F32)

    pl.semaphore_wait(barrier, 31 + 7 + 6)

    def columns(chunk):
        return slice(chunk * HALF, (chunk + 1) * HALF)

    def halo(t, chunk, way):
        slot = (t + 2) % 2
        if way == 0:
            src, dst, target = send_l, from_above, down
        else:
            src, dst, target = send_g, from_below, up
        return pltpu.make_async_remote_copy(
            src_ref=src.at[slot, chunk],
            dst_ref=dst.at[slot, chunk],
            send_sem=halo_send.at[slot, chunk, way],
            recv_sem=halo_recv.at[slot, chunk, way],
            device_id=(target, orb),
            device_id_type=MESH,
        )

    for chunk in range(2):
        send_l[1, chunk] = vbuf[0, REG_L:REG_G, columns(chunk)]
        halo(-1, chunk, 0).start()

    q[...] = one_hot(cell_pos, (KP, KP), 0)
    xs_rows = a_ref[...]
    high, low = split2(xs_rows)
    ah[...] = jnp.zeros(ah.shape, BF16)
    al[...] = jnp.zeros(al.shape, BF16)
    ah[0:CELL, 0:CELL] = high
    al[0:CELL, 0:CELL] = low
    bh[...] = dot(q[...], ah[...]).astype(BF16)
    bl[...] = dot(q[...], al[...]).astype(BF16)
    mh[...] = dot_nt(bh[...], q[...]).astype(BF16)
    ml[...] = dot_nt(bl[...], q[...]).astype(BF16)

    reg_row = iota((REG, HALF), 0)
    mask = jnp.where(reg_row >= 7, 1.0, 0.0).astype(F32) * has_above

    def put(chunk, low_row, high_row, value):
        high, low = split2(value)
        vcat[chunk, low_row:high_row, 0:HALF] = high
        vcat[chunk, low_row:high_row, HALF:W] = low

    def product(chunk, rows, depth):
        both = dot(mh[rows, depth], vcat[chunk, depth, :])
        third = dot(ml[rows, depth], vcat[chunk, depth, 0:HALF])
        return (both[:, 0:HALF] + both[:, HALF:W]) + third

    def prepare(chunk):
        pre[chunk] = product(chunk, slice(INT, REG_END), slice(0, CUT))

    for chunk in range(2):
        put(chunk, 0, KP, vbuf[0, :, columns(chunk)])
        prepare(chunk)

    def faces_out(t, chunk):
        value = pre[chunk] + product(chunk, slice(INT, REG_END), slice(CUT, KP))
        pf[chunk] = value
        slot = (t + 2) % 2
        send_l[slot, chunk] = value[0:REG]
        send_g[slot, chunk] = value[REG : 2 * REG]
        halo(t, chunk, 0).start()
        halo(t, chunk, 1).start()

    def interior(t, chunk):
        now, old = t % 2, (t + 1) % 2
        total = product(chunk, slice(0, INT), slice(0, KP))
        cols = columns(chunk)
        fresh = (total - CENTRE * vbuf[now, 0:INT, cols]) * chosen(t, 0) - chosen(t, 1) * vbuf[old, 0:INT, cols]
        vbuf[old, 0:INT, cols] = fresh
        put(chunk, 0, INT, fresh)

    def faces_in(t, chunk):
        now, old = t % 2, (t + 1) % 2
        slot = t % 2
        halo(t, chunk, 0).wait_recv()
        halo(t, chunk, 1).wait_recv()
        cols = columns(chunk)
        lower = pf[chunk, 0:REG] + from_below[slot, chunk] * has_below
        upper = (pf[chunk, REG : 2 * REG] + from_above[slot, chunk]) * mask
        for rows, total in ((slice(REG_L, REG_G), lower), (slice(REG_G, REG_END), upper)):
            fresh = (total - CENTRE * vbuf[now, rows, cols]) * chosen(t, 0) - chosen(t, 1) * vbuf[old, rows, cols]
            vbuf[old, rows, cols] = fresh
            put(chunk, rows.start, rows.stop, fresh)

    def close(t):
        for chunk in range(2):
            halo(t, chunk, 0).wait_send()
            halo(t, chunk, 1).wait_send()

    for chunk in range(2):
        halo(-1, chunk, 0).wait_recv()
        ghost = from_above[1, chunk] * mask
        vbuf[0, REG_G:REG_END, columns(chunk)] = ghost
        put(chunk, REG_G, REG_END, ghost)
        faces_out(0, chunk)
    for chunk in range(2):
        interior(0, chunk)
        prepare(chunk)
    for chunk in range(2):
        halo(-1, chunk, 0).wait_send()
    close(0)

    def step(t, _):
        for chunk in range(2):
            faces_in(t - 1, chunk)
            faces_out(t, chunk)
        for chunk in range(2):
            interior(t, chunk)
            prepare(chunk)
        close(t)
        return 0

    lax.fori_loop(1, DEGREE, step, 0)
    for chunk in range(2):
        faces_in(DEGREE - 1, chunk)

    fall[0, 0:OWN, :] = vbuf[DEGREE % 2, 0:OWN, :]
    own = fall[0, 0:OWN, :]
    nown[0] = jnp.sum(own * own, axis=0, keepdims=True)
    norms[node] = nown[0]

    def norm_copy(k):
        return pltpu.make_async_remote_copy(
            src_ref=nown.at[0],
            dst_ref=norms.at[node],
            send_sem=n_send,
            recv_sem=n_recv,
            device_id=((node + k) % 32, orb),
            device_id_type=MESH,
        )

    def norm_start(k, _):
        norm_copy(k).start()
        return 0

    lax.fori_loop(1, 32, norm_start, 0)

    first, second = slice(0, PART), slice(PART, OWN)
    first_a, first_b = slice(0, 160), slice(160, PART)
    second_a, second_b = slice(PART, 488), slice(488, OWN)

    def z_copy(index):
        src, dst, rows, da = (
            (0, 6, first, 1),
            (0, 2, second, 3),
            (6, 4, first, 1),
            (2, 4, second, 3),
            (0, 6, second_a, 1),
            (0, 2, first_a, 3),
            (0, 6, second_b, 1),
            (0, 2, first_b, 3),
        )[index]
        return pltpu.make_async_remote_copy(
            src_ref=fall.at[src, rows],
            dst_ref=fall.at[dst, rows],
            send_sem=z_send.at[index],
            recv_sem=z_recv.at[index],
            device_id=(node, orb_at(da, 0)),
            device_id_type=MESH,
        )

    def d_copy(index):
        slot, rows = (
            (0, slice(0, OWN)),
            (6, first),
            (2, second),
            (4, first),
            (4, second),
            (6, second),
            (2, first),
        )[index]
        return pltpu.make_async_remote_copy(
            src_ref=fall.at[slot, rows],
            dst_ref=fall.at[slot + 1, rows],
            send_sem=d_send.at[index],
            recv_sem=d_recv.at[index],
            device_id=(node, orb_at(0, 1)),
            device_id_type=MESH,
        )

    z_copy(0).start()
    z_copy(1).start()
    d_copy(0).start()
    for k in range(8):
        fall[k, OWN:ROWS, :] = jnp.zeros((ROWS - OWN, W), F32)
    stage_h[...] = jnp.zeros(stage_h.shape, BF16)
    stage_l[...] = jnp.zeros(stage_l.shape, BF16)

    padded = (384, W)
    top = jnp.where(iota(padded, 0) < PART, fall[0, 0:384, :], 0.0)
    ta_h[...], ta_l[...] = split2(top.T)
    xs[...] = jnp.zeros(xs.shape, F32)
    xs[0 : OWN - PART, :] = fall[0, PART:OWN, :]
    tb_h[...], tb_l[...] = split2(xs[0:384, :].T)

    def half_gram(which, slot):
        rows = first if which == 0 else second
        high, low = split2(fall[slot, rows, :])
        count = rows.stop - rows.start
        stage_h[which, 0:count, :] = high
        stage_l[which, 0:count, :] = low
        left_h, left_l = (ta_h, ta_l) if which == 0 else (tb_h, tb_l)
        return (dot(left_h[...], stage_h[which]) + dot(left_h[...], stage_l[which])) + dot(left_l[...], stage_h[which])

    FLAT = {0: 0, 1: 1, 6: 2}

    def keep(tile, value):
        if tile in FLAT:
            flat[FLAT[tile]] = value.reshape(16, 16, W)
        else:
            cube[tile - 2] = value.reshape(2, 2, 2, 2, 16, W)

    def rs_copy(group, k):
        lo, hi = ((0, 2), (2, 3))[group]
        to = [(bits[d] + k // 2**d) % 2 for d in range(4)]
        return pltpu.make_async_remote_copy(
            src_ref=flat.at[lo:hi, number(to)],
            dst_ref=flat_in.at[lo:hi, sid],
            send_sem=rs_send.at[group],
            recv_sem=rs_recv.at[group],
            device_id=(node_of(to), orb),
            device_id_type=MESH,
        )

    def rs_start(group):
        def one(k, _):
            rs_copy(group, k).start()
            return 0

        lax.fori_loop(1, 16, one, 0)

    def rs_bytes(group):
        lo, hi = ((0, 2), (2, 3))[group]
        return flat_in.at[lo:hi, 0:15]

    def rs_sum(group):
        whole = rs_bytes(group)
        pltpu.make_async_copy(whole, whole, rs_recv.at[group]).wait()
        for tile, index in FLAT.items():
            if (index == 2) == (group == 1):
                flat_in[index, sid] = flat[index, sid]
                mine[tile] = jnp.sum(flat_in[index], axis=0)

    def cube_index(values):
        return tuple(slice(None) if values[d] is None else values[d] for d in (3, 2, 1, 0))

    def neighbour(d):
        to = list(bits)
        to[d] = 1 - bits[d]
        return (node_of(to), orb)

    def halving(h, j):
        order = [(h + i) % 4 for i in range(4)]
        src, dst = [None] * 4, [None] * 4
        for i in range(j):
            src[order[i]], dst[order[i]] = bits[order[i]], 1 - bits[order[i]]
        src[order[j]] = dst[order[j]] = 1 - bits[order[j]]
        return pltpu.make_async_remote_copy(
            src_ref=cube.at[(h,) + cube_index(src)],
            dst_ref=cube_in.at[(h,) + cube_index(dst)],
            send_sem=c_send.at[h, j],
            recv_sem=c_recv.at[h, j],
            device_id=neighbour(order[j]),
            device_id_type=MESH,
        )

    def halving_in(h, j):
        order = [(h + i) % 4 for i in range(4)]
        halving(h, j).wait_recv()
        kept, came = [None] * 4, [None] * 4
        for i in range(j):
            kept[order[i]], came[order[i]] = bits[order[i]], 1 - bits[order[i]]
        kept[order[j]] = came[order[j]] = bits[order[j]]
        kept, came = (h,) + cube_index(kept), (h,) + cube_index(came)
        if j < 3:
            cube[kept] = cube[kept] + cube_in[came]
        else:
            mine[h + 2] = cube[kept] + cube_in[came]

    def doubling(tile, j):
        order = [(tile + i) % 4 for i in range(4)]
        which = [None] * 4
        for i in range(j, 4):
            which[order[i]] = bits[order[i]]
        where = (tile,) + cube_index(which)
        return pltpu.make_async_remote_copy(
            src_ref=gathered.at[where],
            dst_ref=gathered.at[where],
            send_sem=g_send.at[tile, j],
            recv_sem=g_recv.at[tile, j],
            device_id=neighbour(order[j]),
            device_id_type=MESH,
        )

    def doubling_start(tiles, j):
        for tile in tiles:
            if j == 0:
                gathered[(tile,) + cube_index(bits)] = final[tile]
            doubling(tile, j).start()

    def doubling_wait(tiles, j):
        for tile in tiles:
            doubling(tile, j).wait_recv()

    cross = jnp.where(a >= 2, 1 - c, c)
    partner = ((a + 2) % 4) * 2 + cross
    late = jnp.where(a >= 2, 1, 0)

    def ex_copies(group):
        lo, hi = ((0, 2), (2, 6), (6, 7))[group]
        copies = [
            pltpu.make_async_remote_copy(
                src_ref=mine.at[lo:hi],
                dst_ref=ex0.at[lo:hi],
                send_sem=ex_send.at[group],
                recv_sem=ex_recv.at[group],
                device_id=(flip, orb),
                device_id_type=MESH,
            )
        ]
        pairs = (
            (),
            ((2, 4, orb_at(3, 0)), (3, 5, orb_at(3, 1)), (4, 2, orb_at(1, 0)), (5, 3, orb_at(1, 1))),
            ((6, 7, partner),),
        )[group]
        for src, dst, who in pairs:
            for near in range(2):
                copies.append(
                    pltpu.make_async_remote_copy(
                        src_ref=mine.at[src],
                        dst_ref=(ex1, ex2)[near].at[dst],
                        send_sem=ex_send.at[2 * dst + near],
                        recv_sem=ex_recv.at[2 * dst + near],
                        device_id=(node if near == 0 else flip, who),
                        device_id_type=MESH,
                    )
                )
        return copies

    def ex_start(group):
        for copy in ex_copies(group):
            copy.start()

    def ex_in(group):
        for copy in ex_copies(group):
            copy.wait_recv()
        for tile in ((0, 1), (2, 3, 4, 5), (6, 7))[group]:
            if tile < 2 or tile == 6:
                final[tile] = mine[tile] + ex0[tile]
            elif tile == 7:
                final[tile] = ex1[tile] + ex2[tile]
            else:
                final[tile] = (mine[tile] + ex0[tile]) + (ex1[tile] + ex2[tile])

    def ag_copy(k):
        to = [(bits[d] + k // 2**d) % 2 for d in range(4)]
        return pltpu.make_async_remote_copy(
            src_ref=final.at[6:8],
            dst_ref=gathered_flat.at[0:2, sid],
            send_sem=ag_send,
            recv_sem=ag_recv,
            device_id=(node_of(to), orb),
            device_id_type=MESH,
        )

    def ag_start(k, _):
        ag_copy(k).start()
        return 0

    keep(0, half_gram(0, 0) + half_gram(1, 0))
    d_copy(0).wait_recv()
    keep(1, half_gram(0, 1) + half_gram(1, 1))
    rs_start(0)

    whole_norms = norms.at[0:31]
    pltpu.make_async_copy(whole_norms, whole_norms, n_recv).wait()
    scales[0] = lax.rsqrt(jnp.sum(norms[...], axis=0) / TOTAL_ROWS + eps_norm)

    def scale_copy(k):
        da, dc = k // 2, k % 2
        return pltpu.make_async_remote_copy(
            src_ref=scales.at[0],
            dst_ref=scales.at[((4 - da) % 4) * 2 + dc],
            send_sem=s_send.at[k],
            recv_sem=s_recv.at[k],
            device_id=(node, orb_at(da, dc)),
            device_id_type=MESH,
        )

    for k in range(1, 8):
        scale_copy(k).start()

    natural = iota((ROWS, 1), 0).astype(F32)
    face_lane = jnp.broadcast_to(face_row, (ROWS, 128))
    lane = iota((ROWS, 128), 1).astype(F32)
    hit = jnp.sum(jnp.where(face_lane == natural, lane + 1.0, 0.0), axis=1, keepdims=True)
    below = jnp.sum(jnp.where(face_lane < natural, 1.0, 0.0), axis=1, keepdims=True)
    back = jnp.where(hit > 0.0, LOW - 1.0 + hit, natural - below)
    qt[...] = one_hot(back, (ROWS, KP), 1)
    rot_h[ROWS:KP, :] = jnp.zeros((KP - ROWS, W), BF16)
    rot_l[ROWS:KP, :] = jnp.zeros((KP - ROWS, W), BF16)

    rs_sum(0)
    ex_start(0)

    z_copy(0).wait_recv()
    z_copy(2).start()
    d_copy(1).start()
    z_copy(1).wait_recv()
    z_copy(3).start()
    d_copy(2).start()
    keep(2, half_gram(0, 6))
    halving(0, 0).start()
    keep(4, half_gram(1, 2).T)
    halving(2, 0).start()
    d_copy(1).wait_recv()
    keep(3, half_gram(0, 7))
    halving(1, 0).start()
    d_copy(2).wait_recv()
    keep(5, half_gram(1, 3).T)
    halving(3, 0).start()
    early, middle = (0, 1), (2, 3, 4, 5)
    ex_in(0)
    doubling_start(early, 0)
    for j in range(4):
        for h in range(4):
            halving_in(h, j)
            if j < 3:
                halving(h, j + 1).start()
        if j == 3:
            ex_start(1)
            z_copy(4).start()
            z_copy(5).start()
        doubling_wait(early, j)
        if j < 3:
            doubling_start(early, j + 1)
        if j == 2:
            z_copy(2).wait_recv()
            d_copy(3).start()
            z_copy(3).wait_recv()
            d_copy(4).start()

    d_copy(3).wait_recv()
    d_copy(4).wait_recv()
    keep(6, half_gram(0, 4 + late) + half_gram(1, 4 + late))
    rs_start(1)

    def rotated(slot, tile, transposed):
        scale = scales[slot]
        left_h, left_l = split2(fall[slot] * (scale * scale))
        source = gathered[tile] if tile < 6 else gathered_flat[tile - 6]
        right_h, right_l = split2(source.reshape(W, W))
        times = dot_nt if transposed else dot
        return (times(left_h, right_h) + times(left_h, right_l)) + times(left_l, right_h)

    for k in range(1, 8):
        scale_copy(k).wait_recv()
    acc[...] = rotated(0, 0, False)
    acc[...] += rotated(1, 1, True)

    ex_in(1)
    doubling_start(middle, 0)
    rs_sum(1)
    ex_start(2)
    z_copy(6).start()
    z_copy(7).start()
    doubling_wait(middle, 0)
    doubling_start(middle, 1)
    doubling_wait(middle, 1)
    doubling_start(middle, 2)
    ex_in(2)
    gathered_flat[0, sid] = final[6]
    gathered_flat[1, sid] = final[7]
    lax.fori_loop(1, 16, ag_start, 0)
    doubling_wait(middle, 2)
    doubling_start(middle, 3)
    z_copy(4).wait_recv()
    z_copy(6).wait_recv()
    d_copy(5).start()
    z_copy(5).wait_recv()
    z_copy(7).wait_recv()
    d_copy(6).start()
    doubling_wait(middle, 3)
    acc[...] += rotated(2, 4, False)
    acc[...] += rotated(6, 2, True)
    d_copy(5).wait_recv()
    acc[...] += rotated(7, 3, True)
    d_copy(6).wait_recv()
    acc[...] += rotated(3, 5, False)
    whole_tiles = gathered_flat.at[0:2, 0:15]
    pltpu.make_async_copy(whole_tiles, whole_tiles, ag_recv).wait()
    acc[...] += rotated(4 + late, 6, True)
    acc[...] += rotated(5 - late, 7, False)
    result = (1.5 * fall[0] - (0.5 / TOTAL_ROWS) * acc[...]) * scales[0]
    high, low = split2(result)
    rot_h[0:ROWS, :] = high
    rot_l[0:ROWS, :] = low
    out = dot(qt[...], rot_h[...]) + dot(qt[...], rot_l[...])
    out_ref[...] = out[0:OWN, :]

    for index in range(8):
        z_copy(index).wait_send()
    for index in range(7):
        d_copy(index).wait_send()
    for k in range(1, 8):
        scale_copy(k).wait_send()
    pltpu.make_async_copy(whole_norms, whole_norms, n_send).wait()
    for group in range(2):
        whole = rs_bytes(group)
        pltpu.make_async_copy(whole, whole, rs_send.at[group]).wait()
    for group in range(3):
        for copy in ex_copies(group):
            copy.wait_send()
    for j in range(4):
        for h in range(4):
            halving(h, j).wait_send()
        for tile in early + middle:
            doubling(tile, j).wait_send()
    pltpu.make_async_copy(whole_tiles, whole_tiles, ag_send).wait()


def body(orbitals, cell_matrix, connectivity, face_nodes):
    vmem = pl.BlockSpec(memory_space=pltpu.VMEM)
    dma = pltpu.SemaphoreType.DMA
    return pl.pallas_call(
        kernel,
        out_shape=jax.ShapeDtypeStruct((OWN, W), F32),
        in_specs=[vmem] * 4,
        out_specs=vmem,
        scratch_shapes=[
            pltpu.VMEM((16, KP), jnp.int32),
            pltpu.VMEM((KP, KP), BF16),
            pltpu.VMEM((KP, KP), BF16),
            pltpu.VMEM((KP, KP), BF16),
            pltpu.VMEM((KP, KP), BF16),
            pltpu.VMEM((KP, KP), BF16),
            pltpu.VMEM((KP, KP), BF16),
            pltpu.VMEM((KP, KP), BF16),
            pltpu.VMEM((ROWS, KP), BF16),
            pltpu.VMEM((2, KP, W), BF16),
            pltpu.VMEM((2, KP, W), F32),
            pltpu.VMEM((KP, W), F32),
            pltpu.VMEM((2, 2 * REG, HALF), F32),
            pltpu.VMEM((2, 2 * REG, HALF), F32),
            pltpu.VMEM((2, 2, REG, HALF), F32),
            pltpu.VMEM((2, 2, REG, HALF), F32),
            pltpu.VMEM((2, 2, REG, HALF), F32),
            pltpu.VMEM((2, 2, REG, HALF), F32),
            pltpu.VMEM((8, ROWS, W), F32),
            pltpu.VMEM((W, 384), BF16),
            pltpu.VMEM((W, 384), BF16),
            pltpu.VMEM((W, 384), BF16),
            pltpu.VMEM((W, 384), BF16),
            pltpu.VMEM((2, 384, W), BF16),
            pltpu.VMEM((2, 384, W), BF16),
            pltpu.VMEM((ROWS, W), F32),
            pltpu.VMEM((KP, W), BF16),
            pltpu.VMEM((KP, W), BF16),
            pltpu.VMEM((3, 16, 16, W), F32),
            pltpu.VMEM((3, 16, 16, W), F32),
            pltpu.VMEM((4, 2, 2, 2, 2, 16, W), F32),
            pltpu.VMEM((4, 2, 2, 2, 2, 16, W), F32),
            pltpu.VMEM((7, 16, W), F32),
            pltpu.VMEM((7, 16, W), F32),
            pltpu.VMEM((8, 16, W), F32),
            pltpu.VMEM((8, 16, W), F32),
            pltpu.VMEM((8, 16, W), F32),
            pltpu.VMEM((6, 2, 2, 2, 2, 16, W), F32),
            pltpu.VMEM((2, 16, 16, W), F32),
            pltpu.VMEM((32, 1, W), F32),
            pltpu.VMEM((1, 1, W), F32),
            pltpu.VMEM((8, 1, W), F32),
            dma((2, 2, 2)),
            dma((2, 2, 2)),
            dma((8,)),
            dma((8,)),
            dma((7,)),
            dma((7,)),
            dma((2,)),
            dma((2,)),
            dma((4, 4)),
            dma((4, 4)),
            dma((6, 4)),
            dma((6, 4)),
            dma((16,)),
            dma((16,)),
            dma,
            dma,
            dma,
            dma,
            dma((8,)),
            dma((8,)),
        ],
        compiler_params=pltpu.CompilerParams(
            collective_id=0, has_side_effects=True, vmem_limit_bytes=60 * 1024 * 1024
        ),
    )(orbitals, cell_matrix[0], connectivity, face_nodes.reshape(1, FACE))


def solution(mesh):
    return jax.shard_map(
        body,
        mesh=mesh,
        in_specs=(P("nodes", "orb"), P("nodes", None, None), P("nodes", None), P("nodes")),
        out_specs=P("nodes", "orb"),
        check_vma=False,
    )
```

```python
import functools

import jax
import jax.numpy as jnp
from jax import lax
from jax.experimental import pallas as pl
from jax.experimental.pallas import tpu as pltpu
from jax.sharding import PartitionSpec as P

DEGREE = 8
lowest = -1.0
cutoff = 1.5
ceiling = 4.5
eps_norm = 1e-06

F32 = jnp.float32
BF16 = jnp.bfloat16
MESH = pl.DeviceIdType.MESH

OWN = 648
CELL = 729
FACE = 81
TOTAL_ROWS = 20736
W = 256
HALF = 128
KP = 768
LOW = 567
REG_L = 560
REG_G = 648
REG = 88
REG_END = 736
INT = 560
CUT = 512
ROWS = 656
SOON = 488
PART = 320


def coefficients():
    half_width = (ceiling - cutoff) / 2.0
    centre = (ceiling + cutoff) / 2.0
    sigma_one = half_width / (lowest - centre)
    table = [(sigma_one / half_width, 0.0)]
    now = sigma_one
    for _ in range(DEGREE - 1):
        nxt = 1.0 / (2.0 / sigma_one - now)
        table.append((2.0 * nxt / half_width, now * nxt))
        now = nxt
    return centre, table


CENTRE, TABLE = coefficients()


def chosen(t, which):
    if isinstance(t, int):
        return TABLE[t][which]
    value = jnp.float32(TABLE[0][which])
    for step in range(1, DEGREE):
        value = jnp.where(t == step, jnp.float32(TABLE[step][which]), value)
    return value


def split2(value):
    high = value.astype(BF16)
    low = (value - high.astype(F32)).astype(BF16)
    return high, low


def dot(left, right):
    return jnp.dot(left, right, preferred_element_type=F32)


def dot_nt(left, right):
    return lax.dot_general(left, right, (((1,), (1,)), ((), ())), preferred_element_type=F32)


def iota(shape, dim):
    return lax.broadcasted_iota(jnp.int32, shape, dim)


def one_hot(position, shape, dim):
    return jnp.where(iota(shape, dim).astype(F32) == position, 1.0, 0.0).astype(BF16)


def kernel(
    x_ref, a_ref, conn_ref, faces_ref, out_ref,
    amat, a_sem, x_sem, irow, q, ah, al, bh, bl, mh, ml, qt, vcat, vbuf, xs, pre, pf,
    send_l, send_g, from_above, from_below,
    fall, ta_h, ta_l, tb_h, tb_l, stage_h, stage_l, acc, rot_h, rot_l,
    left_h, left_l, own_out,
    flat, flat_in, cube, cube_in0, cube_in1, mine, ex0, ex1, ex2, final, gathered, norms, nown, scales,
    halo_send, halo_recv, z_send, z_recv, d_send, d_recv,
    rs_send, rs_recv, c_send, c_recv, g_send, g_recv, ex_send, ex_recv, n_send, n_recv, s_send, s_recv,
):
    node = lax.axis_index("nodes")
    orb = lax.axis_index("orb")
    a = orb // 2
    c = orb % 2
    zl = (node // 4) % 2
    x, y = node % 4, node // 8
    bits = ((x // 2 + x % 2) % 2, x // 2, (y // 2 + y % 2) % 2, y // 2)
    flip = node + 4 - 8 * zl
    up = (node + 1) % 32
    down = (node + 31) % 32
    has_above = jnp.where(node < 31, jnp.float32(1.0), jnp.float32(0.0))
    has_below = jnp.where(node > 0, jnp.float32(1.0), jnp.float32(0.0))

    def orb_at(da, dc):
        other = c if dc == 0 else 1 - c
        return ((a + da) % 4) * 2 + other

    def number(corner):
        return corner[3] * 8 + corner[2] * 4 + corner[1] * 2 + corner[0]

    def node_of(corner):
        there_x = corner[1] * 2 + (corner[0] + corner[1]) % 2
        there_y = corner[3] * 2 + (corner[2] + corner[3]) % 2
        return there_y * 8 + zl * 4 + there_x

    sid = number(bits)

    matrix_copy = pltpu.make_async_copy(a_ref, amat, a_sem)
    orbitals_copy = pltpu.make_async_copy(x_ref, xs.at[0:OWN], x_sem)
    orbitals_copy.start()
    matrix_copy.start()
    from_above[...] = jnp.zeros(from_above.shape, F32)
    from_below[...] = jnp.zeros(from_below.shape, F32)

    barrier = pltpu.get_barrier_semaphore()

    def greet(k, _):
        pl.semaphore_signal(barrier, inc=1, device_id=((node + k) % 32, orb), device_id_type=MESH)
        return 0

    lax.fori_loop(1, 32, greet, 0)
    for k in range(1, 8):
        pl.semaphore_signal(barrier, inc=1, device_id=(node, orb_at(k // 2, k % 2)), device_id_type=MESH)
    for k in range(2, 8):
        pl.semaphore_signal(barrier, inc=1, device_id=(flip, orb_at(k // 2, k % 2)), device_id_type=MESH)

    irow[...] = jnp.full(irow.shape, 100000, jnp.int32)
    irow[0:1, 0:FACE] = faces_ref[...]
    face_row = irow[0:1, 0:128].astype(F32)
    irow[8:9, 0:CELL] = conn_ref[...]
    entry = irow[8:9, :].astype(F32)
    square = (128, 128)
    face_col = jnp.sum(
        jnp.where(iota(square, 0) == iota(square, 1), jnp.broadcast_to(face_row, square), 0.0), axis=1, keepdims=True
    )

    def position_row(number):
        shape = (128, KP)
        same = number == face_col
        hit = jnp.sum(jnp.where(same, iota(shape, 0).astype(F32) + 1.0, 0.0), axis=0, keepdims=True)
        below = jnp.sum(jnp.where(face_col < number, 1.0, 0.0), axis=0, keepdims=True)
        return jnp.where(hit > 0.0, LOW - 1.0 + hit, number - below)

    local = iota((1, KP), 1).astype(F32)
    local_pos = jnp.where(local < OWN, position_row(local), -1.0)
    cell_pos = jnp.where(entry < OWN, position_row(entry), jnp.where(entry < CELL, entry + 7.0, -1.0))

    q[...] = one_hot(local_pos, (KP, KP), 0)
    xs[OWN:KP, :] = jnp.zeros((KP - OWN, W), F32)
    orbitals_copy.wait()
    start = xs[...]
    x1 = start.astype(BF16)
    rest = start - x1.astype(F32)
    x2 = rest.astype(BF16)
    x3 = (rest - x2.astype(F32)).astype(BF16)
    vbuf[0, ...] = (dot(q[...], x1) + dot(q[...], x2)) + dot(q[...], x3)
    vbuf[1, ...] = jnp.zeros((KP, W), F32)

    q[...] = one_hot(cell_pos, (KP, KP), 0)
    matrix_copy.wait()
    high, low = split2(amat[...])
    ah[...] = jnp.zeros(ah.shape, BF16)
    al[...] = jnp.zeros(al.shape, BF16)
    ah[0:CELL, 0:CELL] = high
    al[0:CELL, 0:CELL] = low
    bh[...] = dot(q[...], ah[...]).astype(BF16)
    bl[...] = dot(q[...], al[...]).astype(BF16)

    pl.semaphore_wait(barrier, 31 + 7 + 6)

    def columns(chunk):
        return slice(chunk * HALF, (chunk + 1) * HALF)

    def halo(t, chunk, way):
        slot = (t + 2) % 2
        if way == 0:
            src, dst, target = send_l, from_above, down
        else:
            src, dst, target = send_g, from_below, up
        return pltpu.make_async_remote_copy(
            src_ref=src.at[slot, chunk],
            dst_ref=dst.at[slot, chunk],
            send_sem=halo_send.at[slot, chunk, way],
            recv_sem=halo_recv.at[slot, chunk, way],
            device_id=(target, orb),
            device_id_type=MESH,
        )

    def there(way):
        return node > 0 if way == 0 else node < 31

    def halo_start(t, chunk, way):
        @pl.when(there(way))
        def _():
            halo(t, chunk, way).start()

    def halo_in(t, chunk, way):
        @pl.when(there(1 - way))
        def _():
            halo(t, chunk, way).wait_recv()

    def halo_out(t, chunk, way):
        @pl.when(there(way))
        def _():
            halo(t, chunk, way).wait_send()

    for chunk in range(2):
        send_l[1, chunk] = vbuf[0, REG_L:REG_G, columns(chunk)]
        halo_start(-1, chunk, 0)

    mh[...] = dot_nt(bh[...], q[...]).astype(BF16)
    ml[...] = dot_nt(bl[...], q[...]).astype(BF16)

    reg_row = iota((REG, HALF), 0)
    mask = jnp.where(reg_row >= 7, 1.0, 0.0).astype(F32) * has_above

    def put(chunk, low_row, high_row, value):
        high, low = split2(value)
        vcat[chunk, low_row:high_row, 0:HALF] = high
        vcat[chunk, low_row:high_row, HALF:W] = low

    def product(chunk, rows, depth):
        both = dot(mh[rows, depth], vcat[chunk, depth, :])
        third = dot(ml[rows, depth], vcat[chunk, depth, 0:HALF])
        return (both[:, 0:HALF] + both[:, HALF:W]) + third

    def prepare(chunk):
        pre[chunk] = product(chunk, slice(INT, REG_END), slice(0, CUT))

    for chunk in range(2):
        put(chunk, 0, KP, vbuf[0, :, columns(chunk)])
        prepare(chunk)

    def faces_out(t, chunk):
        value = pre[chunk] + product(chunk, slice(INT, REG_END), slice(CUT, KP))
        pf[chunk] = value
        slot = (t + 2) % 2
        send_l[slot, chunk] = value[0:REG]
        send_g[slot, chunk] = value[REG : 2 * REG]
        halo_start(t, chunk, 0)
        halo_start(t, chunk, 1)

    def interior(t, chunk):
        now, old = t % 2, (t + 1) % 2
        total = product(chunk, slice(0, INT), slice(0, KP))
        cols = columns(chunk)
        fresh = (total - CENTRE * vbuf[now, 0:INT, cols]) * chosen(t, 0) - chosen(t, 1) * vbuf[old, 0:INT, cols]
        vbuf[old, 0:INT, cols] = fresh
        put(chunk, 0, INT, fresh)

    def faces_in(t, chunk):
        now, old = t % 2, (t + 1) % 2
        slot = t % 2
        halo_in(t, chunk, 0)
        halo_in(t, chunk, 1)
        cols = columns(chunk)
        lower = pf[chunk, 0:REG] + from_below[slot, chunk] * has_below
        upper = (pf[chunk, REG : 2 * REG] + from_above[slot, chunk]) * mask
        for rows, total in ((slice(REG_L, REG_G), lower), (slice(REG_G, REG_END), upper)):
            fresh = (total - CENTRE * vbuf[now, rows, cols]) * chosen(t, 0) - chosen(t, 1) * vbuf[old, rows, cols]
            vbuf[old, rows, cols] = fresh
            put(chunk, rows.start, rows.stop, fresh)

    def close(t):
        for chunk in range(2):
            halo_out(t, chunk, 0)
            halo_out(t, chunk, 1)

    for chunk in range(2):
        halo_in(-1, chunk, 0)
        ghost = from_above[1, chunk] * mask
        vbuf[0, REG_G:REG_END, columns(chunk)] = ghost
        put(chunk, REG_G, REG_END, ghost)
        faces_out(0, chunk)
    for chunk in range(2):
        interior(0, chunk)
        prepare(chunk)
    for chunk in range(2):
        halo_out(-1, chunk, 0)
    close(0)

    def step(t, _):
        for chunk in range(2):
            faces_in(t - 1, chunk)
            faces_out(t, chunk)
        for chunk in range(2):
            interior(t, chunk)
            prepare(chunk)
        close(t)
        return 0

    lax.fori_loop(1, DEGREE, step, 0)

    first, second = slice(0, PART), slice(PART, OWN)
    first_a, first_b = slice(0, 160), slice(160, PART)
    second_a, second_b = slice(PART, SOON), slice(SOON, OWN)
    hops = (
        (0, 6, first_a, 1),
        (0, 6, first_b, 1),
        (0, 2, second_a, 3),
        (0, 2, second_b, 3),
        (6, 4, first_a, 1),
        (6, 4, first_b, 1),
        (2, 4, second_a, 3),
        (2, 4, second_b, 3),
        (0, 6, slice(320, 440), 1),
        (0, 6, slice(440, 560), 1),
        (0, 6, slice(560, OWN), 1),
        (0, 2, slice(0, 120), 3),
        (0, 2, slice(120, 240), 3),
        (0, 2, slice(240, 320), 3),
    )
    crossings = (
        (0, slice(0, SOON)),
        (0, slice(SOON, OWN)),
        (6, first),
        (2, second),
        (4, first),
        (4, second),
        (6, second),
        (2, first),
    )

    def z_copy(index):
        src, dst, rows, da = hops[index]
        return pltpu.make_async_remote_copy(
            src_ref=fall.at[src, rows],
            dst_ref=fall.at[dst, rows],
            send_sem=z_send.at[index],
            recv_sem=z_recv.at[index],
            device_id=(node, orb_at(da, 0)),
            device_id_type=MESH,
        )

    def d_copy(index):
        slot, rows = crossings[index]
        return pltpu.make_async_remote_copy(
            src_ref=fall.at[slot, rows],
            dst_ref=fall.at[slot + 1, rows],
            send_sem=d_send.at[index],
            recv_sem=d_recv.at[index],
            device_id=(node, orb_at(0, 1)),
            device_id_type=MESH,
        )

    def z_in(*indices):
        for index in indices:
            z_copy(index).wait_recv()

    fall[0, 0:SOON, :] = vbuf[DEGREE % 2, 0:SOON, :]
    d_copy(0).start()
    d_copy(0).wait_recv()
    for index in (0, 2, 1):
        z_copy(index).start()
    for chunk in range(2):
        faces_in(DEGREE - 1, chunk)
    fall[0, SOON:OWN, :] = vbuf[DEGREE % 2, SOON:OWN, :]
    z_copy(3).start()
    d_copy(1).start()
    own = fall[0, 0:OWN, :]
    nown[0] = jnp.sum(own * own, axis=0, keepdims=True)
    norms[node] = nown[0]

    def norm_copy(k):
        return pltpu.make_async_remote_copy(
            src_ref=nown.at[0],
            dst_ref=norms.at[node],
            send_sem=n_send,
            recv_sem=n_recv,
            device_id=((node + k) % 32, orb),
            device_id_type=MESH,
        )

    def norm_start(k, _):
        norm_copy(k).start()
        return 0

    lax.fori_loop(1, 32, norm_start, 0)

    for k in range(8):
        fall[k, OWN:ROWS, :] = jnp.zeros((ROWS - OWN, W), F32)
    stage_h[...] = jnp.zeros(stage_h.shape, BF16)
    stage_l[...] = jnp.zeros(stage_l.shape, BF16)

    padded = (384, W)
    top = jnp.where(iota(padded, 0) < PART, fall[0, 0:384, :], 0.0)
    ta_h[...], ta_l[...] = split2(top.T)
    xs[...] = jnp.zeros(xs.shape, F32)
    xs[0 : OWN - PART, :] = fall[0, PART:OWN, :]
    tb_h[...], tb_l[...] = split2(xs[0:384, :].T)

    def half_gram(which, slot):
        rows = first if which == 0 else second
        high, low = split2(fall[slot, rows, :])
        count = rows.stop - rows.start
        stage_h[which, 0:count, :] = high
        stage_l[which, 0:count, :] = low
        left_h, left_l = (ta_h, ta_l) if which == 0 else (tb_h, tb_l)
        return (dot(left_h[...], stage_h[which]) + dot(left_h[...], stage_l[which])) + dot(left_l[...], stage_h[which])

    def keep(tile, value):
        if tile == 6:
            flat[...] = value.reshape(16, 16, W)
        else:
            cube[tile] = value.reshape(2, 2, 2, 2, 16, W)

    def rs_copy(k):
        to = [(bits[d] + k // 2**d) % 2 for d in range(4)]
        return pltpu.make_async_remote_copy(
            src_ref=flat.at[number(to)],
            dst_ref=flat_in.at[sid],
            send_sem=rs_send,
            recv_sem=rs_recv,
            device_id=(node_of(to), orb),
            device_id_type=MESH,
        )

    def rs_start():
        def one(k, _):
            rs_copy(k).start()
            return 0

        lax.fori_loop(1, 16, one, 0)

    def rs_sum():
        whole = flat_in.at[0:15]
        pltpu.make_async_copy(whole, whole, rs_recv).wait()
        flat_in[sid] = flat[sid]
        mine[6] = jnp.sum(flat_in[...], axis=0)

    def cube_index(values):
        return tuple(slice(None) if values[d] is None else values[d] for d in (3, 2, 1, 0))

    def rounds(tile):
        return ((0, 2), (1, 3)) if tile % 2 == 0 else ((1, 3), (0, 2))

    def peer(pair, way):
        to = list(bits)
        for d, flips in zip(pair, (way % 2, way // 2)):
            if flips:
                to[d] = 1 - bits[d]
        return to

    def halving(h, j, way):
        pairs = rounds(h)
        to = peer(pairs[j], way)
        src = [None] * 4
        for earlier in pairs[:j]:
            for d in earlier:
                src[d] = bits[d]
        for d in pairs[j]:
            src[d] = to[d]
        free = pairs[1 - j] if j == 0 else ()
        piece = tuple(src[d] if d not in free else None for d in range(4))
        return pltpu.make_async_remote_copy(
            src_ref=cube.at[(h,) + cube_index(piece)],
            dst_ref=(cube_in0 if j == 0 else cube_in1).at[(h, way - 1)],
            send_sem=c_send.at[h, j, way - 1],
            recv_sem=c_recv.at[h, j, way - 1],
            device_id=(node_of(to), orb),
            device_id_type=MESH,
        )

    def halving_start(h, j):
        for way in (3, 1, 2):
            halving(h, j, way).start()

    def halving_in(h, j):
        for way in (1, 2, 3):
            halving(h, j, way).wait_recv()
        pairs = rounds(h)
        kept = [None] * 4
        for done in pairs[: j + 1]:
            for d in done:
                kept[d] = bits[d]
        kept = (h,) + cube_index(kept)
        came = cube_in0 if j == 0 else cube_in1
        total = (cube[kept] + came[h, 0]) + (came[h, 1] + came[h, 2])
        if j == 0:
            cube[kept] = total
        else:
            mine[h] = total

    def doubling(tile, j, way):
        pairs = rounds(tile)
        which = [None] * 4
        for later in pairs[j:]:
            for d in later:
                which[d] = bits[d]
        where = (tile,) + cube_index(which)
        return pltpu.make_async_remote_copy(
            src_ref=gathered.at[where],
            dst_ref=gathered.at[where],
            send_sem=g_send.at[tile, j, way - 1],
            recv_sem=g_recv.at[tile, j, way - 1],
            device_id=(node_of(peer(pairs[j], way)), orb),
            device_id_type=MESH,
        )

    def doubling_start(tiles, j):
        for tile in tiles:
            if j == 0:
                gathered[(tile,) + cube_index(bits)] = final[tile]
            for way in (3, 1, 2):
                doubling(tile, j, way).start()

    def doubling_wait(tiles, j):
        for tile in tiles:
            for way in (1, 2, 3):
                doubling(tile, j, way).wait_recv()

    cross = jnp.where(a >= 2, 1 - c, c)
    partner = ((a + 2) % 4) * 2 + cross
    late = jnp.where(a >= 2, 1, 0)

    def ex_copies(group):
        lo, hi = ((0, 2), (2, 6), (6, 7))[group]
        copies = [
            pltpu.make_async_remote_copy(
                src_ref=mine.at[lo:hi],
                dst_ref=ex0.at[lo:hi],
                send_sem=ex_send.at[group],
                recv_sem=ex_recv.at[group],
                device_id=(flip, orb),
                device_id_type=MESH,
            )
        ]
        pairs = (
            (),
            ((2, 4, orb_at(3, 0)), (3, 5, orb_at(3, 1)), (4, 2, orb_at(1, 0)), (5, 3, orb_at(1, 1))),
            ((6, 7, partner),),
        )[group]
        for src, dst, who in pairs:
            for near in range(2):
                copies.append(
                    pltpu.make_async_remote_copy(
                        src_ref=mine.at[src],
                        dst_ref=(ex1, ex2)[near].at[dst],
                        send_sem=ex_send.at[2 * dst + near],
                        recv_sem=ex_recv.at[2 * dst + near],
                        device_id=(node if near == 0 else flip, who),
                        device_id_type=MESH,
                    )
                )
        return copies

    def ex_start(group):
        for copy in ex_copies(group):
            copy.start()

    def ex_in(group):
        for copy in ex_copies(group):
            copy.wait_recv()
        for tile in ((0, 1), (2, 3, 4, 5), (6, 7))[group]:
            if tile < 2 or tile == 6:
                final[tile] = mine[tile] + ex0[tile]
            elif tile == 7:
                final[tile] = ex1[tile] + ex2[tile]
            else:
                final[tile] = (mine[tile] + ex0[tile]) + (ex1[tile] + ex2[tile])

    keep(0, half_gram(0, 0) + half_gram(1, 0))
    halving_start(0, 0)
    d_copy(1).wait_recv()
    keep(1, half_gram(0, 1) + half_gram(1, 1))
    halving_start(1, 0)

    natural = iota((ROWS, 1), 0).astype(F32)
    face_lane = jnp.broadcast_to(face_row, (ROWS, 128))
    lane = iota((ROWS, 128), 1).astype(F32)
    hit = jnp.sum(jnp.where(face_lane == natural, lane + 1.0, 0.0), axis=1, keepdims=True)
    below = jnp.sum(jnp.where(face_lane < natural, 1.0, 0.0), axis=1, keepdims=True)
    back = jnp.where(hit > 0.0, LOW - 1.0 + hit, natural - below)
    qt[...] = one_hot(back, (ROWS, KP), 1)
    rot_h[ROWS:KP, :] = jnp.zeros((KP - ROWS, W), BF16)
    rot_l[ROWS:KP, :] = jnp.zeros((KP - ROWS, W), BF16)

    z_in(0)
    z_copy(4).start()
    z_in(2)
    z_copy(6).start()
    for tile in (0, 1):
        halving_in(tile, 0)
        halving_start(tile, 1)
    for tile in (0, 1):
        halving_in(tile, 1)
    ex_start(0)
    z_in(1)
    z_copy(5).start()
    d_copy(2).start()
    z_in(3)
    z_copy(7).start()
    d_copy(3).start()
    keep(2, half_gram(0, 6))
    halving_start(2, 0)
    keep(4, half_gram(1, 2).T)
    halving_start(4, 0)
    d_copy(2).wait_recv()
    keep(3, half_gram(0, 7))
    halving_start(3, 0)
    d_copy(3).wait_recv()
    keep(5, half_gram(1, 3).T)
    halving_start(5, 0)

    whole_norms = norms.at[0:31]
    pltpu.make_async_copy(whole_norms, whole_norms, n_recv).wait()
    scales[0] = lax.rsqrt(jnp.sum(norms[...], axis=0) / TOTAL_ROWS + eps_norm)

    def scale_copy(k):
        da, dc = k // 2, k % 2
        return pltpu.make_async_remote_copy(
            src_ref=scales.at[0],
            dst_ref=scales.at[((4 - da) % 4) * 2 + dc],
            send_sem=s_send.at[k],
            recv_sem=s_recv.at[k],
            device_id=(node, orb_at(da, dc)),
            device_id_type=MESH,
        )

    for k in range(1, 8):
        scale_copy(k).start()

    def laid_out(slot):
        scale = scales[slot]
        value = fall[slot] if slot == 0 else fall[slot] * (scale * scale)
        high, low = split2(value)
        rot_h[0:ROWS, :] = high
        rot_l[0:ROWS, :] = low
        return dot(qt[...], rot_h[...]), dot(qt[...], rot_l[...])

    def lay_out(slot):
        high, low = laid_out(slot)
        left_h[slot] = high.astype(BF16)
        left_l[slot] = low.astype(BF16)

    def rotated(slot, tile, transposed):
        right_h, right_l = split2(gathered[tile].reshape(W, W))
        times = dot_nt if transposed else dot
        return (times(left_h[slot], right_h) + times(left_h[slot], right_l)) + times(left_l[slot], right_h)

    early, middle, last = (0, 1), (2, 3, 4, 5), (6, 7)
    for tile in middle:
        halving_in(tile, 0)
        halving_start(tile, 1)
    z_copy(8).start()
    z_copy(11).start()
    scale_copy(1).wait_recv()
    high, low = laid_out(0)
    own_out[...] = (high + low) * (1.5 * scales[0])
    square_own = scales[0] * scales[0]
    high, low = split2((high + low) * square_own)
    left_h[0] = high
    left_l[0] = low
    lay_out(1)
    for tile in middle:
        halving_in(tile, 1)
    ex_start(1)
    z_copy(9).start()
    z_copy(12).start()
    ex_in(0)
    doubling_start(early, 0)
    z_in(4, 5)
    d_copy(4).start()
    z_in(6, 7)
    d_copy(5).start()
    d_copy(4).wait_recv()
    d_copy(5).wait_recv()
    keep(6, half_gram(0, 4 + late) + half_gram(1, 4 + late))
    rs_start()
    doubling_wait(early, 0)
    doubling_start(early, 1)
    ex_in(1)
    doubling_start(middle, 0)
    for k in range(2, 8):
        scale_copy(k).wait_recv()
    lay_out(4)
    lay_out(5)
    rs_sum()
    ex_start(2)
    z_copy(10).start()
    z_copy(13).start()
    doubling_wait(middle, 0)
    doubling_start(middle, 1)
    doubling_wait(early, 1)
    acc[...] = rotated(0, 0, False)
    acc[...] += rotated(1, 1, True)
    ex_in(2)
    doubling_start(last, 0)
    z_in(8, 9, 10)
    d_copy(6).start()
    z_in(11, 12, 13)
    d_copy(7).start()
    lay_out(2)
    lay_out(6)
    doubling_wait(last, 0)
    doubling_start(last, 1)
    d_copy(6).wait_recv()
    lay_out(7)
    d_copy(7).wait_recv()
    lay_out(3)
    doubling_wait(middle, 1)
    acc[...] += rotated(2, 4, False)
    acc[...] += rotated(6, 2, True)
    acc[...] += rotated(7, 3, True)
    acc[...] += rotated(3, 5, False)
    doubling_wait(last, 1)
    acc[...] += rotated(4 + late, 6, True)
    acc[...] += rotated(5 - late, 7, False)
    result = own_out[...] - acc[...] * ((0.5 / TOTAL_ROWS) * scales[0])
    out_ref[...] = result[0:OWN, :]

    for index in range(14):
        z_copy(index).wait_send()
    for index in range(8):
        d_copy(index).wait_send()
    for k in range(1, 8):
        scale_copy(k).wait_send()
    pltpu.make_async_copy(whole_norms, whole_norms, n_send).wait()
    sent = flat_in.at[0:15]
    pltpu.make_async_copy(sent, sent, rs_send).wait()
    for group in range(3):
        for copy in ex_copies(group):
            copy.wait_send()
    for j in range(2):
        for way in (1, 2, 3):
            for tile in range(6):
                halving(tile, j, way).wait_send()
            for tile in range(8):
                doubling(tile, j, way).wait_send()


def body(orbitals, cell_matrix, connectivity, face_nodes):
    vmem = pl.BlockSpec(memory_space=pltpu.VMEM)
    anywhere = pl.BlockSpec(memory_space=pl.ANY)
    dma = pltpu.SemaphoreType.DMA
    return pl.pallas_call(
        kernel,
        out_shape=jax.ShapeDtypeStruct((OWN, W), F32),
        in_specs=[anywhere, anywhere, vmem, vmem],
        out_specs=vmem,
        scratch_shapes=[
            pltpu.VMEM((CELL, CELL), F32),
            dma,
            dma,
            pltpu.VMEM((16, KP), jnp.int32),
            pltpu.VMEM((KP, KP), BF16),
            pltpu.VMEM((KP, KP), BF16),
            pltpu.VMEM((KP, KP), BF16),
            pltpu.VMEM((KP, KP), BF16),
            pltpu.VMEM((KP, KP), BF16),
            pltpu.VMEM((KP, KP), BF16),
            pltpu.VMEM((KP, KP), BF16),
            pltpu.VMEM((ROWS, KP), BF16),
            pltpu.VMEM((2, KP, W), BF16),
            pltpu.VMEM((2, KP, W), F32),
            pltpu.VMEM((KP, W), F32),
            pltpu.VMEM((2, 2 * REG, HALF), F32),
            pltpu.VMEM((2, 2 * REG, HALF), F32),
            pltpu.VMEM((2, 2, REG, HALF), F32),
            pltpu.VMEM((2, 2, REG, HALF), F32),
            pltpu.VMEM((2, 2, REG, HALF), F32),
            pltpu.VMEM((2, 2, REG, HALF), F32),
            pltpu.VMEM((8, ROWS, W), F32),
            pltpu.VMEM((W, 384), BF16),
            pltpu.VMEM((W, 384), BF16),
            pltpu.VMEM((W, 384), BF16),
            pltpu.VMEM((W, 384), BF16),
            pltpu.VMEM((2, 384, W), BF16),
            pltpu.VMEM((2, 384, W), BF16),
            pltpu.VMEM((ROWS, W), F32),
            pltpu.VMEM((KP, W), BF16),
            pltpu.VMEM((KP, W), BF16),
            pltpu.VMEM((8, ROWS, W), BF16),
            pltpu.VMEM((8, ROWS, W), BF16),
            pltpu.VMEM((ROWS, W), F32),
            pltpu.VMEM((16, 16, W), F32),
            pltpu.VMEM((16, 16, W), F32),
            pltpu.VMEM((6, 2, 2, 2, 2, 16, W), F32),
            pltpu.VMEM((6, 3, 2, 2, 16, W), F32),
            pltpu.VMEM((6, 3, 16, W), F32),
            pltpu.VMEM((7, 16, W), F32),
            pltpu.VMEM((7, 16, W), F32),
            pltpu.VMEM((8, 16, W), F32),
            pltpu.VMEM((8, 16, W), F32),
            pltpu.VMEM((8, 16, W), F32),
            pltpu.VMEM((8, 2, 2, 2, 2, 16, W), F32),
            pltpu.VMEM((32, 1, W), F32),
            pltpu.VMEM((1, 1, W), F32),
            pltpu.VMEM((8, 1, W), F32),
            dma((2, 2, 2)),
            dma((2, 2, 2)),
            dma((14,)),
            dma((14,)),
            dma((8,)),
            dma((8,)),
            dma,
            dma,
            dma((6, 2, 3)),
            dma((6, 2, 3)),
            dma((8, 2, 3)),
            dma((8, 2, 3)),
            dma((16,)),
            dma((16,)),
            dma,
            dma,
            dma((8,)),
            dma((8,)),
        ],
        compiler_params=pltpu.CompilerParams(
            collective_id=0, has_side_effects=True, vmem_limit_bytes=60 * 1024 * 1024
        ),
    )(orbitals, cell_matrix[0], connectivity, face_nodes.reshape(1, FACE))


def solution(mesh):
    return jax.shard_map(
        body,
        mesh=mesh,
        in_specs=(P("nodes", "orb"), P("nodes", None, None), P("nodes", None), P("nodes")),
        out_specs=P("nodes", "orb"),
        check_vma=False,
    )
```

```python
import functools

import jax
import jax.numpy as jnp
from jax import lax
from jax.experimental import pallas as pl
from jax.experimental.pallas import tpu as pltpu
from jax.sharding import PartitionSpec as P

DEGREE = 8
lowest = -1.0
cutoff = 1.5
ceiling = 4.5
eps_norm = 1e-06

F32 = jnp.float32
BF16 = jnp.bfloat16
MESH = pl.DeviceIdType.MESH

OWN = 648
CELL = 729
FACE = 81
TOTAL_ROWS = 20736
W = 256
HALF = 128
KP = 768
LOW = 567
REG_L = 560
REG_G = 648
REG = 88
REG_END = 736
INT = 560
CUT = 512
ROWS = 656
SOON = 488
PART = 320


def coefficients():
    half_width = (ceiling - cutoff) / 2.0
    centre = (ceiling + cutoff) / 2.0
    sigma_one = half_width / (lowest - centre)
    table = [(sigma_one / half_width, 0.0)]
    now = sigma_one
    for _ in range(DEGREE - 1):
        nxt = 1.0 / (2.0 / sigma_one - now)
        table.append((2.0 * nxt / half_width, now * nxt))
        now = nxt
    return centre, table


CENTRE, TABLE = coefficients()


def chosen(t, which):
    if isinstance(t, int):
        return TABLE[t][which]
    value = jnp.float32(TABLE[0][which])
    for step in range(1, DEGREE):
        value = jnp.where(t == step, jnp.float32(TABLE[step][which]), value)
    return value


def split2(value):
    high = value.astype(BF16)
    low = (value - high.astype(F32)).astype(BF16)
    return high, low


def dot(left, right):
    return jnp.dot(left, right, preferred_element_type=F32)


def dot_nt(left, right):
    return lax.dot_general(left, right, (((1,), (1,)), ((), ())), preferred_element_type=F32)


def iota(shape, dim):
    return lax.broadcasted_iota(jnp.int32, shape, dim)


def one_hot(position, shape, dim):
    return jnp.where(iota(shape, dim).astype(F32) == position, 1.0, 0.0).astype(BF16)


def kernel(
    x_ref, a_ref, conn_ref, faces_ref, out_ref,
    amat, a_sem, x_sem, irow, q, ah, al, bh, bl, mh, ml, qt, vcat, vbuf, xs, pre, pf,
    send_l, send_g, from_above, from_below,
    fall, ta_h, ta_l, tb_h, tb_l, stage_h, stage_l, acc, rot_h, rot_l,
    left_h, left_l, own_out,
    flat, flat_in, cube, cube_in0, cube_in1, mine, ex0, ex1, ex2, final, gathered, norms, nown, scales,
    halo_send, halo_recv, z_send, z_recv, d_send, d_recv,
    rs_send, rs_recv, c_send, c_recv, g_send, g_recv, ex_send, ex_recv, n_send, n_recv, s_send, s_recv,
):
    node = lax.axis_index("nodes")
    orb = lax.axis_index("orb")
    a = orb // 2
    c = orb % 2
    zl = (node // 4) % 2
    x, y = node % 4, node // 8
    bits = ((x // 2 + x % 2) % 2, x // 2, (y // 2 + y % 2) % 2, y // 2)
    flip = node + 4 - 8 * zl
    up = (node + 1) % 32
    down = (node + 31) % 32
    has_above = jnp.where(node < 31, jnp.float32(1.0), jnp.float32(0.0))
    has_below = jnp.where(node > 0, jnp.float32(1.0), jnp.float32(0.0))

    def orb_at(da, dc):
        other = c if dc == 0 else 1 - c
        return ((a + da) % 4) * 2 + other

    def number(corner):
        return corner[3] * 8 + corner[2] * 4 + corner[1] * 2 + corner[0]

    def node_of(corner):
        there_x = corner[1] * 2 + (corner[0] + corner[1]) % 2
        there_y = corner[3] * 2 + (corner[2] + corner[3]) % 2
        return there_y * 8 + zl * 4 + there_x

    sid = number(bits)

    matrix_copy = pltpu.make_async_copy(a_ref, amat, a_sem)
    orbitals_copy = pltpu.make_async_copy(x_ref, xs.at[0:OWN], x_sem)
    orbitals_copy.start()
    matrix_copy.start()
    from_above[...] = jnp.zeros(from_above.shape, F32)
    from_below[...] = jnp.zeros(from_below.shape, F32)

    barrier = pltpu.get_barrier_semaphore()

    def greet(k, _):
        pl.semaphore_signal(barrier, inc=1, device_id=((node + k) % 32, orb), device_id_type=MESH)
        return 0

    lax.fori_loop(1, 32, greet, 0)
    for k in range(1, 8):
        pl.semaphore_signal(barrier, inc=1, device_id=(node, orb_at(k // 2, k % 2)), device_id_type=MESH)
    for k in range(2, 8):
        pl.semaphore_signal(barrier, inc=1, device_id=(flip, orb_at(k // 2, k % 2)), device_id_type=MESH)

    irow[...] = jnp.full(irow.shape, 100000, jnp.int32)
    irow[0:1, 0:FACE] = faces_ref[...]
    face_row = irow[0:1, 0:128].astype(F32)
    irow[8:9, 0:CELL] = conn_ref[...]
    entry = irow[8:9, :].astype(F32)
    square = (128, 128)
    face_col = jnp.sum(
        jnp.where(iota(square, 0) == iota(square, 1), jnp.broadcast_to(face_row, square), 0.0), axis=1, keepdims=True
    )

    def position_row(number):
        shape = (128, KP)
        same = number == face_col
        hit = jnp.sum(jnp.where(same, iota(shape, 0).astype(F32) + 1.0, 0.0), axis=0, keepdims=True)
        below = jnp.sum(jnp.where(face_col < number, 1.0, 0.0), axis=0, keepdims=True)
        return jnp.where(hit > 0.0, LOW - 1.0 + hit, number - below)

    local = iota((1, KP), 1).astype(F32)
    local_pos = jnp.where(local < OWN, position_row(local), -1.0)
    cell_pos = jnp.where(entry < OWN, position_row(entry), jnp.where(entry < CELL, entry + 7.0, -1.0))

    q[...] = one_hot(local_pos, (KP, KP), 0)
    xs[OWN:KP, :] = jnp.zeros((KP - OWN, W), F32)
    orbitals_copy.wait()
    start = xs[...]
    x1 = start.astype(BF16)
    rest = start - x1.astype(F32)
    x2 = rest.astype(BF16)
    x3 = (rest - x2.astype(F32)).astype(BF16)
    vbuf[0, ...] = (dot(q[...], x1) + dot(q[...], x2)) + dot(q[...], x3)
    vbuf[1, ...] = jnp.zeros((KP, W), F32)

    q[...] = one_hot(cell_pos, (KP, KP), 0)
    matrix_copy.wait()
    high, low = split2(amat[...])
    ah[...] = jnp.zeros(ah.shape, BF16)
    al[...] = jnp.zeros(al.shape, BF16)
    ah[0:CELL, 0:CELL] = high
    al[0:CELL, 0:CELL] = low
    bh[...] = dot(q[...], ah[...]).astype(BF16)
    bl[...] = dot(q[...], al[...]).astype(BF16)

    pl.semaphore_wait(barrier, 31 + 7 + 6)

    def columns(chunk):
        return slice(chunk * HALF, (chunk + 1) * HALF)

    def halo(t, chunk, way):
        slot = (t + 2) % 2
        if way == 0:
            src, dst, target = send_l, from_above, down
        else:
            src, dst, target = send_g, from_below, up
        return pltpu.make_async_remote_copy(
            src_ref=src.at[slot, chunk],
            dst_ref=dst.at[slot, chunk],
            send_sem=halo_send.at[slot, chunk, way],
            recv_sem=halo_recv.at[slot, chunk, way],
            device_id=(target, orb),
            device_id_type=MESH,
        )

    def there(way):
        return node > 0 if way == 0 else node < 31

    def halo_start(t, chunk, way):
        @pl.when(there(way))
        def _():
            halo(t, chunk, way).start()

    def halo_in(t, chunk, way):
        @pl.when(there(1 - way))
        def _():
            halo(t, chunk, way).wait_recv()

    def halo_out(t, chunk, way):
        @pl.when(there(way))
        def _():
            halo(t, chunk, way).wait_send()

    for chunk in range(2):
        send_l[1, chunk] = vbuf[0, REG_L:REG_G, columns(chunk)]
        halo_start(-1, chunk, 0)

    mh[...] = dot_nt(bh[...], q[...]).astype(BF16)
    ml[...] = dot_nt(bl[...], q[...]).astype(BF16)

    reg_row = iota((REG, HALF), 0)
    mask = jnp.where(reg_row >= 7, 1.0, 0.0).astype(F32) * has_above

    def put(chunk, low_row, high_row, value):
        high, low = split2(value)
        vcat[chunk, low_row:high_row, 0:HALF] = high
        vcat[chunk, low_row:high_row, HALF:W] = low

    def product(chunk, rows, depth):
        both = dot(mh[rows, depth], vcat[chunk, depth, :])
        third = dot(ml[rows, depth], vcat[chunk, depth, 0:HALF])
        return (both[:, 0:HALF] + both[:, HALF:W]) + third

    def prepare(chunk):
        pre[chunk] = product(chunk, slice(INT, REG_END), slice(0, CUT))

    for chunk in range(2):
        put(chunk, 0, KP, vbuf[0, :, columns(chunk)])
        prepare(chunk)

    def faces_out(t, chunk):
        value = pre[chunk] + product(chunk, slice(INT, REG_END), slice(CUT, KP))
        pf[chunk] = value
        slot = (t + 2) % 2
        send_l[slot, chunk] = value[0:REG]
        send_g[slot, chunk] = value[REG : 2 * REG]
        halo_start(t, chunk, 0)
        halo_start(t, chunk, 1)

    def interior(t, chunk):
        now, old = t % 2, (t + 1) % 2
        total = product(chunk, slice(0, INT), slice(0, KP))
        cols = columns(chunk)
        fresh = (total - CENTRE * vbuf[now, 0:INT, cols]) * chosen(t, 0) - chosen(t, 1) * vbuf[old, 0:INT, cols]
        vbuf[old, 0:INT, cols] = fresh
        put(chunk, 0, INT, fresh)

    def faces_in(t, chunk):
        now, old = t % 2, (t + 1) % 2
        slot = t % 2
        halo_in(t, chunk, 0)
        halo_in(t, chunk, 1)
        cols = columns(chunk)
        lower = pf[chunk, 0:REG] + from_below[slot, chunk] * has_below
        upper = (pf[chunk, REG : 2 * REG] + from_above[slot, chunk]) * mask
        for rows, total in ((slice(REG_L, REG_G), lower), (slice(REG_G, REG_END), upper)):
            fresh = (total - CENTRE * vbuf[now, rows, cols]) * chosen(t, 0) - chosen(t, 1) * vbuf[old, rows, cols]
            vbuf[old, rows, cols] = fresh
            put(chunk, rows.start, rows.stop, fresh)

    def close(t):
        for chunk in range(2):
            halo_out(t, chunk, 0)
            halo_out(t, chunk, 1)

    for chunk in range(2):
        halo_in(-1, chunk, 0)
        ghost = from_above[1, chunk] * mask
        vbuf[0, REG_G:REG_END, columns(chunk)] = ghost
        put(chunk, REG_G, REG_END, ghost)
        faces_out(0, chunk)
    for chunk in range(2):
        interior(0, chunk)
        prepare(chunk)
    for chunk in range(2):
        halo_out(-1, chunk, 0)
    close(0)

    def step(t, _):
        for chunk in range(2):
            faces_in(t - 1, chunk)
            faces_out(t, chunk)
        for chunk in range(2):
            interior(t, chunk)
            prepare(chunk)
        close(t)
        return 0

    lax.fori_loop(1, DEGREE, step, 0)

    first, second = slice(0, PART), slice(PART, OWN)
    first_a, first_b = slice(0, 160), slice(160, PART)
    second_a, second_b = slice(PART, SOON), slice(SOON, OWN)
    hops = (
        (0, 6, first_a, 1),
        (0, 6, first_b, 1),
        (0, 2, second_a, 3),
        (0, 2, second_b, 3),
        (6, 4, first_a, 1),
        (6, 4, first_b, 1),
        (2, 4, second_a, 3),
        (2, 4, second_b, 3),
        (0, 6, slice(320, 440), 1),
        (0, 6, slice(440, 560), 1),
        (0, 6, slice(560, OWN), 1),
        (0, 2, slice(0, 120), 3),
        (0, 2, slice(120, 240), 3),
        (0, 2, slice(240, 320), 3),
    )
    crossings = (
        (0, slice(0, SOON)),
        (0, slice(SOON, OWN)),
        (6, first),
        (2, second),
        (4, first),
        (4, second),
        (6, second),
        (2, first),
    )

    def z_copy(index):
        src, dst, rows, da = hops[index]
        return pltpu.make_async_remote_copy(
            src_ref=fall.at[src, rows],
            dst_ref=fall.at[dst, rows],
            send_sem=z_send.at[index],
            recv_sem=z_recv.at[index],
            device_id=(node, orb_at(da, 0)),
            device_id_type=MESH,
        )

    def d_copy(index):
        slot, rows = crossings[index]
        return pltpu.make_async_remote_copy(
            src_ref=fall.at[slot, rows],
            dst_ref=fall.at[slot + 1, rows],
            send_sem=d_send.at[index],
            recv_sem=d_recv.at[index],
            device_id=(node, orb_at(0, 1)),
            device_id_type=MESH,
        )

    def z_in(*indices):
        for index in indices:
            z_copy(index).wait_recv()

    fall[0, 0:SOON, :] = vbuf[DEGREE % 2, 0:SOON, :]
    d_copy(0).start()
    d_copy(0).wait_recv()
    for index in (0, 2, 1):
        z_copy(index).start()
    for chunk in range(2):
        faces_in(DEGREE - 1, chunk)
    fall[0, SOON:OWN, :] = vbuf[DEGREE % 2, SOON:OWN, :]
    z_copy(3).start()
    d_copy(1).start()
    own = fall[0, 0:OWN, :]
    nown[0] = jnp.sum(own * own, axis=0, keepdims=True)
    norms[node] = nown[0]

    def norm_copy(k):
        return pltpu.make_async_remote_copy(
            src_ref=nown.at[0],
            dst_ref=norms.at[node],
            send_sem=n_send,
            recv_sem=n_recv,
            device_id=((node + k) % 32, orb),
            device_id_type=MESH,
        )

    def norm_start(k, _):
        norm_copy(k).start()
        return 0

    lax.fori_loop(1, 32, norm_start, 0)

    for k in range(8):
        fall[k, OWN:ROWS, :] = jnp.zeros((ROWS - OWN, W), F32)
    stage_h[...] = jnp.zeros(stage_h.shape, BF16)
    stage_l[...] = jnp.zeros(stage_l.shape, BF16)

    padded = (384, W)
    top = jnp.where(iota(padded, 0) < PART, fall[0, 0:384, :], 0.0)
    ta_h[...], ta_l[...] = split2(top.T)
    xs[...] = jnp.zeros(xs.shape, F32)
    xs[0 : OWN - PART, :] = fall[0, PART:OWN, :]
    tb_h[...], tb_l[...] = split2(xs[0:384, :].T)

    def half_gram(which, slot):
        rows = first if which == 0 else second
        high, low = split2(fall[slot, rows, :])
        count = rows.stop - rows.start
        stage_h[which, 0:count, :] = high
        stage_l[which, 0:count, :] = low
        left_h, left_l = (ta_h, ta_l) if which == 0 else (tb_h, tb_l)
        return (dot(left_h[...], stage_h[which]) + dot(left_h[...], stage_l[which])) + dot(left_l[...], stage_h[which])

    def keep(tile, value):
        if tile == 6:
            flat[...] = value.reshape(16, 16, W)
        else:
            cube[tile] = value.reshape(2, 2, 2, 2, 16, W)

    def rs_copy(k):
        to = [(bits[d] + k // 2**d) % 2 for d in range(4)]
        return pltpu.make_async_remote_copy(
            src_ref=flat.at[number(to)],
            dst_ref=flat_in.at[sid],
            send_sem=rs_send,
            recv_sem=rs_recv,
            device_id=(node_of(to), orb),
            device_id_type=MESH,
        )

    def rs_start():
        def one(k, _):
            rs_copy(k).start()
            return 0

        lax.fori_loop(1, 16, one, 0)

    def rs_sum():
        whole = flat_in.at[0:15]
        pltpu.make_async_copy(whole, whole, rs_recv).wait()
        flat_in[sid] = flat[sid]
        mine[6] = jnp.sum(flat_in[...], axis=0)

    def cube_index(values):
        return tuple(slice(None) if values[d] is None else values[d] for d in (3, 2, 1, 0))

    def rounds(tile):
        return ((0, 2), (1, 3)) if tile % 2 == 0 else ((1, 3), (0, 2))

    def peer(pair, way):
        to = list(bits)
        for d, flips in zip(pair, (way % 2, way // 2)):
            if flips:
                to[d] = 1 - bits[d]
        return to

    def halving(h, j, way):
        pairs = rounds(h)
        to = peer(pairs[j], way)
        src = [None] * 4
        for earlier in pairs[:j]:
            for d in earlier:
                src[d] = bits[d]
        for d in pairs[j]:
            src[d] = to[d]
        free = pairs[1 - j] if j == 0 else ()
        piece = tuple(src[d] if d not in free else None for d in range(4))
        return pltpu.make_async_remote_copy(
            src_ref=cube.at[(h,) + cube_index(piece)],
            dst_ref=(cube_in0 if j == 0 else cube_in1).at[(h, way - 1)],
            send_sem=c_send.at[h, j, way - 1],
            recv_sem=c_recv.at[h, j, way - 1],
            device_id=(node_of(to), orb),
            device_id_type=MESH,
        )

    def halving_start(h, j):
        for way in (3, 1, 2):
            halving(h, j, way).start()

    def halving_in(h, j):
        for way in (1, 2, 3):
            halving(h, j, way).wait_recv()
        pairs = rounds(h)
        kept = [None] * 4
        for done in pairs[: j + 1]:
            for d in done:
                kept[d] = bits[d]
        kept = (h,) + cube_index(kept)
        came = cube_in0 if j == 0 else cube_in1
        total = (cube[kept] + came[h, 0]) + (came[h, 1] + came[h, 2])
        if j == 0:
            cube[kept] = total
        else:
            mine[h] = total

    def doubling(tile, j, way):
        pairs = rounds(tile)
        which = [None] * 4
        for later in pairs[j:]:
            for d in later:
                which[d] = bits[d]
        where = (tile,) + cube_index(which)
        return pltpu.make_async_remote_copy(
            src_ref=gathered.at[where],
            dst_ref=gathered.at[where],
            send_sem=g_send.at[tile, j, way - 1],
            recv_sem=g_recv.at[tile, j, way - 1],
            device_id=(node_of(peer(pairs[j], way)), orb),
            device_id_type=MESH,
        )

    def doubling_start(tiles, j):
        for tile in tiles:
            if j == 0:
                gathered[(tile,) + cube_index(bits)] = final[tile]
            for way in (3, 1, 2):
                doubling(tile, j, way).start()

    def doubling_wait(tiles, j):
        for tile in tiles:
            for way in (1, 2, 3):
                doubling(tile, j, way).wait_recv()

    cross = jnp.where(a >= 2, 1 - c, c)
    partner = ((a + 2) % 4) * 2 + cross
    late = jnp.where(a >= 2, 1, 0)

    def ex_copies(group):
        lo, hi = ((0, 2), (2, 6), (6, 7))[group]
        copies = [
            pltpu.make_async_remote_copy(
                src_ref=mine.at[lo:hi],
                dst_ref=ex0.at[lo:hi],
                send_sem=ex_send.at[group],
                recv_sem=ex_recv.at[group],
                device_id=(flip, orb),
                device_id_type=MESH,
            )
        ]
        pairs = (
            (),
            ((2, 4, orb_at(3, 0)), (3, 5, orb_at(3, 1)), (4, 2, orb_at(1, 0)), (5, 3, orb_at(1, 1))),
            ((6, 7, partner),),
        )[group]
        for src, dst, who in pairs:
            for near in range(2):
                copies.append(
                    pltpu.make_async_remote_copy(
                        src_ref=mine.at[src],
                        dst_ref=(ex1, ex2)[near].at[dst],
                        send_sem=ex_send.at[2 * dst + near],
                        recv_sem=ex_recv.at[2 * dst + near],
                        device_id=(node if near == 0 else flip, who),
                        device_id_type=MESH,
                    )
                )
        return copies

    def ex_start(group):
        for copy in ex_copies(group):
            copy.start()

    def ex_in(group):
        for copy in ex_copies(group):
            copy.wait_recv()
        for tile in ((0, 1), (2, 3, 4, 5), (6, 7))[group]:
            if tile < 2 or tile == 6:
                final[tile] = mine[tile] + ex0[tile]
            elif tile == 7:
                final[tile] = ex1[tile] + ex2[tile]
            else:
                final[tile] = (mine[tile] + ex0[tile]) + (ex1[tile] + ex2[tile])

    keep(0, half_gram(0, 0) + half_gram(1, 0))
    halving_start(0, 0)
    d_copy(1).wait_recv()
    keep(1, half_gram(0, 1) + half_gram(1, 1))
    halving_start(1, 0)

    natural = iota((ROWS, 1), 0).astype(F32)
    face_lane = jnp.broadcast_to(face_row, (ROWS, 128))
    lane = iota((ROWS, 128), 1).astype(F32)
    hit = jnp.sum(jnp.where(face_lane == natural, lane + 1.0, 0.0), axis=1, keepdims=True)
    below = jnp.sum(jnp.where(face_lane < natural, 1.0, 0.0), axis=1, keepdims=True)
    back = jnp.where(hit > 0.0, LOW - 1.0 + hit, natural - below)
    qt[...] = one_hot(back, (ROWS, KP), 1)
    rot_h[ROWS:KP, :] = jnp.zeros((KP - ROWS, W), BF16)
    rot_l[ROWS:KP, :] = jnp.zeros((KP - ROWS, W), BF16)

    z_in(0)
    z_copy(4).start()
    z_in(2)
    z_copy(6).start()
    for tile in (0, 1):
        halving_in(tile, 0)
        halving_start(tile, 1)
    for tile in (0, 1):
        halving_in(tile, 1)
    ex_start(0)
    z_in(1)
    z_copy(5).start()
    d_copy(2).start()
    z_in(3)
    z_copy(7).start()
    d_copy(3).start()
    z_copy(8).start()
    z_copy(11).start()
    keep(2, half_gram(0, 6))
    halving_start(2, 0)
    keep(4, half_gram(1, 2).T)
    halving_start(4, 0)
    d_copy(2).wait_recv()
    keep(3, half_gram(0, 7))
    halving_start(3, 0)
    d_copy(3).wait_recv()
    keep(5, half_gram(1, 3).T)
    halving_start(5, 0)

    whole_norms = norms.at[0:31]
    pltpu.make_async_copy(whole_norms, whole_norms, n_recv).wait()
    scales[0] = lax.rsqrt(jnp.sum(norms[...], axis=0) / TOTAL_ROWS + eps_norm)

    def scale_copy(k):
        da, dc = k // 2, k % 2
        return pltpu.make_async_remote_copy(
            src_ref=scales.at[0],
            dst_ref=scales.at[((4 - da) % 4) * 2 + dc],
            send_sem=s_send.at[k],
            recv_sem=s_recv.at[k],
            device_id=(node, orb_at(da, dc)),
            device_id_type=MESH,
        )

    for k in range(1, 8):
        scale_copy(k).start()

    def laid_out(slot):
        scale = scales[slot]
        value = fall[slot] if slot == 0 else fall[slot] * (scale * scale)
        high, low = split2(value)
        rot_h[0:ROWS, :] = high
        rot_l[0:ROWS, :] = low
        return dot(qt[...], rot_h[...]), dot(qt[...], rot_l[...])

    def lay_out(slot):
        high, low = laid_out(slot)
        left_h[slot] = high.astype(BF16)
        left_l[slot] = low.astype(BF16)

    def rotated(slot, tile, transposed):
        right_h, right_l = split2(gathered[tile].reshape(W, W))
        times = dot_nt if transposed else dot
        return (times(left_h[slot], right_h) + times(left_h[slot], right_l)) + times(left_l[slot], right_h)

    early, middle, last = (0, 1), (2, 3, 4, 5), (6, 7)
    for tile in middle:
        halving_in(tile, 0)
        halving_start(tile, 1)
    z_in(4, 5)
    d_copy(4).start()
    z_in(6, 7)
    d_copy(5).start()
    for tile in middle:
        halving_in(tile, 1)
    ex_start(1)
    z_copy(9).start()
    z_copy(12).start()
    d_copy(4).wait_recv()
    d_copy(5).wait_recv()
    keep(6, half_gram(0, 4 + late) + half_gram(1, 4 + late))
    rs_start()
    ex_in(0)
    doubling_start(early, 0)
    scale_copy(1).wait_recv()
    high, low = laid_out(0)
    own_out[...] = (high + low) * (1.5 * scales[0])
    square_own = scales[0] * scales[0]
    high, low = split2((high + low) * square_own)
    left_h[0] = high
    left_l[0] = low
    lay_out(1)
    doubling_wait(early, 0)
    doubling_start(early, 1)
    ex_in(1)
    doubling_start(middle, 0)
    rs_sum()
    ex_start(2)
    z_copy(10).start()
    z_copy(13).start()
    for k in range(2, 8):
        scale_copy(k).wait_recv()
    lay_out(4)
    lay_out(5)
    doubling_wait(middle, 0)
    doubling_start(middle, 1)
    doubling_wait(early, 1)
    acc[...] = rotated(0, 0, False)
    acc[...] += rotated(1, 1, True)
    ex_in(2)
    doubling_start(last, 0)
    z_in(8, 9, 10)
    d_copy(6).start()
    z_in(11, 12, 13)
    d_copy(7).start()
    lay_out(2)
    lay_out(6)
    doubling_wait(last, 0)
    doubling_start(last, 1)
    d_copy(6).wait_recv()
    lay_out(7)
    d_copy(7).wait_recv()
    lay_out(3)
    doubling_wait(middle, 1)
    acc[...] += rotated(2, 4, False)
    acc[...] += rotated(6, 2, True)
    acc[...] += rotated(7, 3, True)
    acc[...] += rotated(3, 5, False)
    doubling_wait(last, 1)
    acc[...] += rotated(4 + late, 6, True)
    acc[...] += rotated(5 - late, 7, False)
    result = own_out[...] - acc[...] * ((0.5 / TOTAL_ROWS) * scales[0])
    out_ref[...] = result[0:OWN, :]

    for index in range(14):
        z_copy(index).wait_send()
    for index in range(8):
        d_copy(index).wait_send()
    for k in range(1, 8):
        scale_copy(k).wait_send()
    pltpu.make_async_copy(whole_norms, whole_norms, n_send).wait()
    sent = flat_in.at[0:15]
    pltpu.make_async_copy(sent, sent, rs_send).wait()
    for group in range(3):
        for copy in ex_copies(group):
            copy.wait_send()
    for j in range(2):
        for way in (1, 2, 3):
            for tile in range(6):
                halving(tile, j, way).wait_send()
            for tile in range(8):
                doubling(tile, j, way).wait_send()


def body(orbitals, cell_matrix, connectivity, face_nodes):
    vmem = pl.BlockSpec(memory_space=pltpu.VMEM)
    anywhere = pl.BlockSpec(memory_space=pl.ANY)
    dma = pltpu.SemaphoreType.DMA
    return pl.pallas_call(
        kernel,
        out_shape=jax.ShapeDtypeStruct((OWN, W), F32),
        in_specs=[anywhere, anywhere, vmem, vmem],
        out_specs=vmem,
        scratch_shapes=[
            pltpu.VMEM((CELL, CELL), F32),
            dma,
            dma,
            pltpu.VMEM((16, KP), jnp.int32),
            pltpu.VMEM((KP, KP), BF16),
            pltpu.VMEM((KP, KP), BF16),
            pltpu.VMEM((KP, KP), BF16),
            pltpu.VMEM((KP, KP), BF16),
            pltpu.VMEM((KP, KP), BF16),
            pltpu.VMEM((KP, KP), BF16),
            pltpu.VMEM((KP, KP), BF16),
            pltpu.VMEM((ROWS, KP), BF16),
            pltpu.VMEM((2, KP, W), BF16),
            pltpu.VMEM((2, KP, W), F32),
            pltpu.VMEM((KP, W), F32),
            pltpu.VMEM((2, 2 * REG, HALF), F32),
            pltpu.VMEM((2, 2 * REG, HALF), F32),
            pltpu.VMEM((2, 2, REG, HALF), F32),
            pltpu.VMEM((2, 2, REG, HALF), F32),
            pltpu.VMEM((2, 2, REG, HALF), F32),
            pltpu.VMEM((2, 2, REG, HALF), F32),
            pltpu.VMEM((8, ROWS, W), F32),
            pltpu.VMEM((W, 384), BF16),
            pltpu.VMEM((W, 384), BF16),
            pltpu.VMEM((W, 384), BF16),
            pltpu.VMEM((W, 384), BF16),
            pltpu.VMEM((2, 384, W), BF16),
            pltpu.VMEM((2, 384, W), BF16),
            pltpu.VMEM((ROWS, W), F32),
            pltpu.VMEM((KP, W), BF16),
            pltpu.VMEM((KP, W), BF16),
            pltpu.VMEM((8, ROWS, W), BF16),
            pltpu.VMEM((8, ROWS, W), BF16),
            pltpu.VMEM((ROWS, W), F32),
            pltpu.VMEM((16, 16, W), F32),
            pltpu.VMEM((16, 16, W), F32),
            pltpu.VMEM((6, 2, 2, 2, 2, 16, W), F32),
            pltpu.VMEM((6, 3, 2, 2, 16, W), F32),
            pltpu.VMEM((6, 3, 16, W), F32),
            pltpu.VMEM((7, 16, W), F32),
            pltpu.VMEM((7, 16, W), F32),
            pltpu.VMEM((8, 16, W), F32),
            pltpu.VMEM((8, 16, W), F32),
            pltpu.VMEM((8, 16, W), F32),
            pltpu.VMEM((8, 2, 2, 2, 2, 16, W), F32),
            pltpu.VMEM((32, 1, W), F32),
            pltpu.VMEM((1, 1, W), F32),
            pltpu.VMEM((8, 1, W), F32),
            dma((2, 2, 2)),
            dma((2, 2, 2)),
            dma((14,)),
            dma((14,)),
            dma((8,)),
            dma((8,)),
            dma,
            dma,
            dma((6, 2, 3)),
            dma((6, 2, 3)),
            dma((8, 2, 3)),
            dma((8, 2, 3)),
            dma((16,)),
            dma((16,)),
            dma,
            dma,
            dma((8,)),
            dma((8,)),
        ],
        compiler_params=pltpu.CompilerParams(
            collective_id=0, has_side_effects=True, vmem_limit_bytes=60 * 1024 * 1024
        ),
    )(orbitals, cell_matrix[0], connectivity, face_nodes.reshape(1, FACE))


def solution(mesh):
    return jax.shard_map(
        body,
        mesh=mesh,
        in_specs=(P("nodes", "orb"), P("nodes", None, None), P("nodes", None), P("nodes")),
        out_specs=P("nodes", "orb"),
        check_vma=False,
    )
```
